32 devices in a mesh: row: 8 (over z, y), col: 4 (over x, core).
Axes of the slice: x: 2, y: 2, z: 4, core: 2. Of those that a mesh axis runs over, the one named last changes fastest.
Arguments:
- embeddings: bfloat16 [12288, 768], P(('row', 'col'))
- doc_order: int32 [12288], P(('row', 'col')), may hold values from 0 to 12287, each once
Outputs:
- nearest_earlier: float32 [12288], P(('row', 'col'))
The draws below stay inside these ranges and needn't reach their ends.
Inputs may be any that keep to these rules, and one draw needn't show every extreme that they name: `doc_order`: each value 0 to 12287 appears once.
All inputs are finite; a program needn't handle non-finite values.
Results may differ from the reference program's by a relative error of at most 0.00051.
Values may be sent and summed in bfloat16 or wider, within the bound.
No kernel may reach another device: no remote copies, remote signals or barrier semaphores. Data moves between devices by JAX's collectives and lax.ppermute only.
A program may use at most 64 MiB of HBM per device.

```python
import jax
import jax.numpy as jnp
from jax import lax

D = 768
N = 12288


def draw_embeddings(key, part):
    groups = max(N // 4, 1)
    key_group = jax.random.fold_in(key, 11)
    key_amp = jax.random.fold_in(key, 12)
    key_center = jax.random.fold_in(key, 13)
    key_noise = jax.random.fold_in(key, 14)
    member = jax.random.randint(key_group, (N,), 0, groups)
    amplitude = jax.random.uniform(key_amp, (groups,), jnp.float32, 0.5, 3.0)
    centers = jax.random.normal(key_center, (groups, D), jnp.float32)
    noise = jax.random.normal(key_noise, (N, D), jnp.float32)
    values = noise + amplitude[member][:, None] * centers[member]
    return values.astype(jnp.bfloat16)


def setup_inputs(seed: int = 0) -> dict:
    streams_of = jax.random.split(jax.random.key(seed), 3)
    embeddings = draw_embeddings(jax.random.fold_in(streams_of[2], 71), 0)
    doc_order = jax.random.permutation(streams_of[1], N).astype(jnp.int32)
    return dict(embeddings=embeddings, doc_order=doc_order)


def normalize_rows(embeddings):
    floats = embeddings.astype(jnp.float32)
    scale = lax.rsqrt(lax.optimization_barrier(jnp.sum(floats * floats, axis=1, keepdims=True)) + 1e-06)
    return (floats * scale).astype(jnp.bfloat16)

def reference(embeddings, doc_order):
    unit_rows = normalize_rows(embeddings)
    block_rows = 1024 if N % 1024 == 0 else N
    row_groups = unit_rows.reshape(N // block_rows, block_rows, D)
    order_groups = doc_order.reshape(N // block_rows, block_rows)

    def one_block(pair):
        rows_here, orders_here = pair
        scores = jnp.dot(rows_here, unit_rows.T, preferred_element_type=jnp.float32)
        earlier = doc_order[None, :] < orders_here[:, None]
        masked = jnp.where(earlier, scores, jnp.float32(-1.0))
        return jnp.maximum(lax.optimization_barrier(jnp.max(masked, axis=1)), jnp.float32(-1.0))
    result = lax.map(one_block, (row_groups, order_groups))
    return result.reshape(N)
```

```python
import functools

import jax
import jax.numpy as jnp
from jax import lax
from jax.experimental import pallas as pl
from jax.experimental.pallas import tpu as pltpu
from jax.sharding import PartitionSpec as P

AXES = ("row", "col")
CORES = 2
PAD = 16
FAR = 1.0e9


class Layout:
    def __init__(self, mesh):
        rows, cols = mesh.shape["row"], mesh.shape["col"]
        self.xs = cols // CORES
        self.ys = self.xs if rows % self.xs == 0 else 1
        self.lines = rows // self.ys

    def index(self, line, y, x, core):
        return ((line * self.ys + y) * self.xs + x) * CORES + core

    def pairs(self, target):
        found = []
        for line in range(self.lines):
            for y in range(self.ys):
                for x in range(self.xs):
                    for core in range(CORES):
                        to = target(line, y, x, core)
                        if to is not None:
                            found.append((self.index(line, y, x, core), self.index(*to)))
        return found

    def plane_move(self, dy, dx):
        return self.pairs(lambda l, y, x, c: (l, (y + dy) % self.ys, (x + dx) % self.xs, c))

    def swap(self):
        return self.pairs(lambda l, y, x, c: (l, y, x, CORES - 1 - c))

    def plane_offsets(self):
        return [(dy, dx) for dy in range(self.ys) for dx in range(self.xs) if dy or dx]

    def line_maps(self):
        maps = []
        for step in range(1, (self.lines + 1) // 2):
            maps.append({i: (i + step) % self.lines for i in range(self.lines)})
        if self.lines % 2 == 0:
            half = self.lines // 2
            maps.append({(i if i % 2 == 0 else i + half): (i + half if i % 2 == 0 else i) for i in range(half)})
        return maps

    def line_move(self, line_map):
        return self.pairs(lambda l, y, x, c: (line_map[l], y, x, c) if l in line_map else None)


def backward(pairs):
    return [(b, a) for a, b in pairs]


def pack_body(emb_ref, order_ref, out_ref):
    n, width = emb_ref.shape
    floats = emb_ref[...].astype(jnp.float32)
    scale = lax.rsqrt(jnp.sum(floats * floats, axis=1, keepdims=True) + 1e-06)
    out_ref[:n, :] = (floats * scale).astype(jnp.bfloat16)
    code = order_ref[...] + 1
    high = (code >> 8).astype(jnp.float32)
    low = (code & 255).astype(jnp.float32)
    line = lax.broadcasted_iota(jnp.int32, (PAD, n), 0)
    tail = jnp.where(line == 0, high, jnp.where(line == 1, low, 0.0))
    out_ref[n:, :] = jnp.zeros((PAD, width), jnp.bfloat16)
    out_ref[n:, :n] = tail.astype(jnp.bfloat16)


def pack(embeddings, doc_order):
    n, width = embeddings.shape
    return pl.pallas_call(
        pack_body,
        out_shape=jax.ShapeDtypeStruct((n + PAD, width), jnp.bfloat16),
        name="pack",
    )(embeddings, doc_order.reshape(1, n))


def lane_orders(ref):
    n = ref.shape[0] - PAD
    tail = ref[n:, :n].astype(jnp.float32)
    order = tail[0:1] * 256.0 + tail[1:2]
    return jnp.where(order == 0.0, FAR, order)


def row_orders(ref):
    n = ref.shape[0] - PAD
    return jnp.broadcast_to(lane_orders(ref), (128, n)).T


def match_body(n_rows, n_cols, two_sided, has_rows, has_cols, chunk, *refs):
    at = 0

    def take(count):
        nonlocal at
        at += count
        return refs[at - count : at]

    rows, cols = take(n_rows), take(n_cols)
    row_in = take(n_rows if has_rows else 0)
    col_in = take(n_cols if has_cols else 0)
    row_out = take(n_rows)
    col_out = take(n_cols if two_sided else 0)
    order_ref, col_acc = take(2)
    n = rows[0].shape[0] - PAD
    lanes = 128
    col_orders = [lane_orders(ref) for ref in cols]
    if two_sided:
        col_acc[...] = jnp.full(col_acc.shape, -1.0, jnp.float32)
    for r in range(n_rows):
        order_ref[...] = row_orders(rows[r])

        def step(i, carry):
            start = pl.multiple_of(i * chunk, chunk)
            mine = rows[r][pl.ds(start, chunk), :]
            own_order = order_ref[pl.ds(start, chunk), 0:1]
            best = jnp.full((chunk, lanes), -1.0, jnp.float32)
            for c in range(n_cols):
                score = lax.dot_general(mine, cols[c][:n, :], (((1,), (1,)), ((), ())), preferred_element_type=jnp.float32)
                earlier = col_orders[c] < own_order
                masked = jnp.where(earlier, score, -1.0)
                for k in range(n // lanes):
                    best = jnp.maximum(best, masked[:, k * lanes : (k + 1) * lanes])
                if two_sided:
                    other = jnp.where(earlier, -1.0, score)
                    col_acc[c] = jnp.maximum(col_acc[c], jnp.max(other.reshape(chunk // 8, 8, n), axis=0))
            row_out[r][0:1, pl.ds(start, chunk)] = jnp.max(best.T, axis=0, keepdims=True)
            return carry

        lax.fori_loop(0, n // chunk, step, 0)
        if has_rows:
            row_out[r][...] = jnp.maximum(row_out[r][...], row_in[r][...])
    if two_sided:
        for c in range(n_cols):
            value = jnp.max(col_acc[c], axis=0, keepdims=True)
            if has_cols:
                value = jnp.maximum(value, col_in[c][...])
            col_out[c][...] = value


def match(name, rows, cols, two_sided, row_in=None, col_in=None):
    n = rows[0].shape[0] - PAD
    line = jax.ShapeDtypeStruct((1, n), jnp.float32)
    body = functools.partial(
        match_body, len(rows), len(cols), two_sided, row_in is not None, col_in is not None, 128 if n % 128 == 0 else n
    )
    outs = pl.pallas_call(
        body,
        out_shape=[line] * (len(rows) + (len(cols) if two_sided else 0)),
        scratch_shapes=[pltpu.VMEM((n, 128), jnp.float32), pltpu.VMEM((len(cols), 8, n), jnp.float32)],
        name=name,
    )(*rows, *cols, *(row_in or ()), *(col_in or ()))
    return outs[: len(rows)], outs[len(rows) :]


def solution(mesh):
    layout = Layout(mesh)

    def send(value, pairs):
        return lax.ppermute(value, AXES, pairs)

    def shards(embeddings, doc_order):
        own = pack(embeddings, doc_order)
        n = embeddings.shape[0]
        swap = layout.swap()
        moves = [layout.line_move(m) for m in layout.line_maps()]
        offsets = [layout.plane_move(*d) for d in layout.plane_offsets()]
        twin = send(own, swap)
        line = [send(own, m) for m in moves]
        plane = [own] + [send(own, m) for m in offsets]
        line_twin = [send(block, swap) for block in line]

        (mine, twins), _ = match("plane", [own, twin], plane, False)
        col_best = None
        row_best = []
        for k, block in enumerate(line):
            rows, col_best = match(f"line{k}", [block, line_twin[k]], plane, True, None, col_best)
            row_best.append(rows)

        back = [mine, send(twins, swap)]
        for (a, b), m in zip(row_best, moves):
            whole = jnp.maximum(a, send(b, swap))
            got = send(whole, backward(m))
            sources = jnp.zeros((layout.index(layout.lines - 1, layout.ys - 1, layout.xs - 1, CORES - 1) + 1,), jnp.bool_)
            sources = sources.at[jnp.array([s for s, _ in m])].set(True)
            here = sources[lax.axis_index(AXES)]
            back.append(jnp.where(here, got, -1.0))
        if col_best is not None:
            back.append(col_best[0])
            for value, m in zip(col_best[1:], offsets):
                back.append(send(value, backward(m)))
        best = functools.reduce(jnp.maximum, back)
        return jnp.maximum(best, -1.0).reshape(n)

    return jax.shard_map(
        shards,
        mesh=mesh,
        in_specs=(P(AXES, None), P(AXES)),
        out_specs=P(AXES),
        check_vma=False,
    )
```

```python
import functools

import jax
import jax.numpy as jnp
from jax import lax
from jax.experimental import pallas as pl
from jax.experimental.pallas import tpu as pltpu
from jax.sharding import PartitionSpec as P

AXES = ("row", "col")
CORES = 2
PAD = 16
FAR = 1.0e9
VMEM_GRANT = 16 << 20


class Layout:
    def __init__(self, mesh):
        rows, cols = mesh.shape["row"], mesh.shape["col"]
        self.xs = cols // CORES
        self.ys = self.xs if rows % self.xs == 0 else 1
        self.lines = rows // self.ys

    def index(self, line, y, x, core):
        return ((line * self.ys + y) * self.xs + x) * CORES + core

    def pairs(self, target):
        found = []
        for line in range(self.lines):
            for y in range(self.ys):
                for x in range(self.xs):
                    for core in range(CORES):
                        to = target(line, y, x, core)
                        if to is not None:
                            found.append((self.index(line, y, x, core), self.index(*to)))
        return found

    def plane_move(self, dy, dx):
        return self.pairs(lambda l, y, x, c: (l, (y + dy) % self.ys, (x + dx) % self.xs, c))

    def swap(self):
        return self.pairs(lambda l, y, x, c: (l, y, x, CORES - 1 - c))

    def plane_offsets(self):
        return [(dy, dx) for dy in range(self.ys) for dx in range(self.xs) if dy or dx]

    def line_maps(self):
        maps = []
        for step in range(1, (self.lines + 1) // 2):
            maps.append({i: (i + step) % self.lines for i in range(self.lines)})
        if self.lines % 2 == 0:
            half = self.lines // 2
            maps.append({(i if i % 2 == 0 else i + half): (i + half if i % 2 == 0 else i) for i in range(half)})
        return maps

    def line_move(self, line_map):
        return self.pairs(lambda l, y, x, c: (line_map[l], y, x, c) if l in line_map else None)

    def line_return(self, line_map):
        back = {b: a for a, b in line_map.items()}
        free = [i for i in range(self.lines) if i not in line_map]
        back.update(zip([i for i in range(self.lines) if i not in back], free))
        return self.line_move(back)


def backward(pairs):
    return [(b, a) for a, b in pairs]


def pack_body(pieces, emb_ref, order_ref, out_ref, *piece_refs):
    n, width = emb_ref.shape
    floats = emb_ref[...].astype(jnp.float32)
    scale = lax.rsqrt(jnp.sum(floats * floats, axis=1, keepdims=True) + 1e-06)
    out_ref[:n, :] = (floats * scale).astype(jnp.bfloat16)
    code = order_ref[...].reshape(1, n) + 1
    high = (code >> 8).astype(jnp.float32)
    low = (code & 255).astype(jnp.float32)
    line = lax.broadcasted_iota(jnp.int32, (PAD, n), 0)
    tail = jnp.where(line == 0, high, jnp.where(line == 1, low, 0.0))
    out_ref[n:, :] = jnp.zeros((PAD, width), jnp.bfloat16)
    out_ref[n:, :n] = tail.astype(jnp.bfloat16)
    for (start, rows), ref in zip(pieces, piece_refs):
        cut(out_ref, start, rows, ref)


def pack(embeddings, doc_order, pieces=()):
    n, width = embeddings.shape
    shapes = [pltpu.VMEM((rows + PAD, width), jnp.bfloat16) for rows in (n, *(rows for _, rows in pieces))]
    call = pl.pallas_call(
        functools.partial(pack_body, pieces),
        out_shape=shapes,
        compiler_params=pltpu.CompilerParams(vmem_limit_bytes=VMEM_GRANT),
        name="pack",
    )
    return call(*in_vmem([embeddings, doc_order]))


def cut(ref, start, rows, out_ref):
    n = ref.shape[0] - PAD
    out_ref[:rows, :] = ref[start : start + rows, :]
    out_ref[rows:, :] = jnp.zeros((PAD, ref.shape[1]), jnp.bfloat16)
    out_ref[rows:, :rows] = ref[n:, start : start + rows]


def piece_body(start, rows, ref, out_ref):
    cut(ref, start, rows, out_ref)


def piece(block, start, rows):
    return pl.pallas_call(
        functools.partial(piece_body, start, rows),
        out_shape=pltpu.VMEM((rows + PAD, block.shape[1]), jnp.bfloat16),
        compiler_params=pltpu.CompilerParams(vmem_limit_bytes=VMEM_GRANT),
        name="piece",
    )(*in_vmem([block]))


def lane_orders(ref):
    n = ref.shape[0] - PAD
    tail = ref[n:, :n].astype(jnp.float32)
    order = tail[0:1] * 256.0 + tail[1:2]
    return jnp.where(order == 0.0, FAR, order)


def match_body(n_rows, n_plain, has_rows, chips, known, *refs):
    at = 0

    def take(count):
        nonlocal at
        at += count
        return refs[at - count : at]

    side_cols = sum(chips)
    rows, cols = take(n_rows), take(2 * side_cols)
    row_in, col_in = take(sum(has_rows)), take(2 * len(known))
    row_out, col_out = take(n_rows), take(2 if n_plain < n_rows else 0)
    (col_acc,) = take(1)
    lanes = 128
    col_orders = [lane_orders(ref) for ref in cols]
    row_in = list(row_in)
    for r in range(n_rows):
        n = rows[r].shape[0] - PAD
        own_orders = lane_orders(rows[r])
        own_order = jnp.broadcast_to(own_orders, (lanes, n)).T[:, 0:1]
        best = jnp.full((n, lanes), -1.0, jnp.float32)
        for c in range(2 * side_cols):
            m = cols[c].shape[0] - PAD
            score = lax.dot_general(
                rows[r][:n, :], cols[c][:m, :], (((1,), (1,)), ((), ())), preferred_element_type=jnp.float32
            )
            earlier = col_orders[c] < own_order
            masked = jnp.where(earlier, score, -1.0)
            for k in range(m // lanes):
                best = jnp.maximum(best, masked[:, k * lanes : (k + 1) * lanes])
            if r >= n_plain:
                other = jnp.max(jnp.where(earlier, -1.0, score).reshape(n // 8, 8, m), axis=0)
                col_acc[c, :, :m] = other if r == n_plain else jnp.maximum(col_acc[c, :, :m], other)
        value = jnp.where(own_orders == FAR, -1.0, jnp.max(best.T, axis=0, keepdims=True))
        if has_rows[r]:
            value = jnp.maximum(value, row_in.pop(0)[...])
        row_out[r][...] = value
    for side in range(len(col_out)):
        before = [col_in[side * len(known) + i][k : k + 1, :] for i in range(len(known)) for k in range(known[i])]
        c = side * side_cols
        for chip in range(len(chips)):
            start = 0
            for _ in range(chips[chip]):
                m = cols[c].shape[0] - PAD
                value = jnp.max(col_acc[c, :, :m], axis=0, keepdims=True)
                if before:
                    value = jnp.maximum(value, before[chip][:, start : start + m])
                col_out[side][chip : chip + 1, start : start + m] = value
                start += m
                c += 1


def in_vmem(values):
    return [pltpu.with_memory_space_constraint(v, pltpu.VMEM) for v in values]


def match(rows, chips, n_plain, row_in=None, col_in=()):
    ours = [block for mine, _ in chips for block in mine]
    twins = [block for _, other in chips for block in other]
    row_in = row_in or [None] * len(rows)
    width = rows[0].shape[1]
    n = sum(block.shape[0] - PAD for block in chips[0][0])
    sizes = [block.shape[0] - PAD for block in rows]
    block = pltpu.VMEM((len(chips), n), jnp.float32)
    before = [pair[0] for pair in col_in] + [pair[1] for pair in col_in]
    call = pl.pallas_call(
        functools.partial(
            match_body,
            len(rows),
            n_plain,
            [value is not None for value in row_in],
            [len(mine) for mine, _ in chips],
            [pair[0].shape[0] for pair in col_in],
        ),
        out_shape=[pltpu.VMEM((1, size), jnp.float32) for size in sizes] + [block, block] * (n_plain < len(rows)),
        scratch_shapes=[pltpu.VMEM((2 * len(ours), 8, n), jnp.float32)],
        cost_estimate=pl.CostEstimate(
            flops=4 * sum(sizes) * len(chips) * n * width,
            bytes_accessed=2 * (sum(sizes) + 2 * len(chips) * n) * width,
            transcendentals=0,
        ),
        compiler_params=pltpu.CompilerParams(vmem_limit_bytes=VMEM_GRANT),
    )
    outs = call(*in_vmem([*rows, *ours, *twins, *(value for value in row_in if value is not None), *before]))
    return outs[: len(rows)], tuple(outs[len(rows) :])


def merge_body(ours_ref, theirs_ref, *out_refs):
    value = jnp.maximum(ours_ref[...], theirs_ref[...])
    for k, ref in enumerate(out_refs):
        ref[...] = value[k : k + 1]


def merge(ours, theirs):
    count, n = ours.shape
    return pl.pallas_call(
        merge_body,
        out_shape=[pltpu.VMEM((1, n), jnp.float32)] * count,
        compiler_params=pltpu.CompilerParams(vmem_limit_bytes=VMEM_GRANT),
        name="merge",
    )(*in_vmem([ours, theirs]))


def solution(mesh):
    layout = Layout(mesh)
    maps = layout.line_maps()
    offsets = layout.plane_offsets()

    def send(value, pairs):
        return lax.ppermute(value, AXES, pairs)

    def nearest(embeddings, doc_order):
        n = embeddings.shape[0]
        last = min(n, 128)
        pieces = ((0, n - last), (n - last, last)) if n > last else ((0, n),)
        swap = layout.swap()
        early, late = maps[:-1], maps[-1]

        raw = [send(embeddings, layout.line_move(m)) for m in early]
        own, *parts = pack(embeddings, doc_order, pieces)
        plane = [send(own, layout.plane_move(*d)) for d in offsets[:-1]]
        half = [send(part, layout.line_move(late)) for part in parts]
        raw_order = [send(doc_order, layout.line_move(m)) for m in early]
        line = [pack(block, order)[0] for block, order in zip(raw, raw_order)]
        near_blocks = [own, *plane]
        near_chips = [([block], [send(block, swap)]) for block in near_blocks]

        dy, dx = offsets[-1]
        routes = [((0, dx), (dy, 0)), ((dy, 0), (0, dx))]
        corner = []
        for k, (start, rows) in enumerate(pieces):
            have, move = routes[k % 2]
            block = piece(plane[offsets.index(have)], start, rows)
            corner.append(send(block, layout.plane_move(*move)))
        far_chips = [(corner, [send(block, swap) for block in corner])]

        first = [own, *line]
        near_rows, near = match(first, near_chips, 1)
        half_rows, near = match(half[:-1], near_chips, 0, None, [near])
        rows, far = match(first + half[:-1], far_chips, 1, [*near_rows, *half_rows])
        last_rows, (ours, theirs) = match(half[-1:], near_chips + far_chips, 0, None, [near, far])

        mine, *answers = rows[: len(first)]
        answers.append(jnp.concatenate([*rows[len(first) :], *last_rows], axis=1))
        back = [mine]
        for value, m in zip(answers, maps):
            back.append(send(value, layout.line_return(m)))
        own_best, *others = merge(ours, send(theirs, swap))
        back.append(own_best)
        for value, d in zip(others, offsets):
            back.append(send(value, backward(layout.plane_move(*d))))
        best = functools.reduce(jnp.maximum, back)
        return jnp.maximum(best, -1.0).reshape(doc_order.shape)

    return jax.shard_map(
        nearest,
        mesh=mesh,
        in_specs=(P(AXES, None), P(AXES)),
        out_specs=P(AXES),
        check_vma=False,
    )
```

```python
import functools

import jax
import jax.numpy as jnp
from jax import lax
from jax.experimental import pallas as pl
from jax.experimental.pallas import tpu as pltpu
from jax.sharding import PartitionSpec as P

AXES = ("row", "col")
CORES = 2
PAD = 16
FAR = 1.0e9
VMEM_GRANT = 16 << 20


class Layout:
    def __init__(self, mesh):
        rows, cols = mesh.shape["row"], mesh.shape["col"]
        self.xs = cols // CORES
        self.ys = self.xs if rows % self.xs == 0 else 1
        self.lines = rows // self.ys

    def index(self, line, y, x, core):
        return ((line * self.ys + y) * self.xs + x) * CORES + core

    def pairs(self, target):
        found = []
        for line in range(self.lines):
            for y in range(self.ys):
                for x in range(self.xs):
                    for core in range(CORES):
                        to = target(line, y, x, core)
                        if to is not None:
                            found.append((self.index(line, y, x, core), self.index(*to)))
        return found

    def plane_move(self, dy, dx):
        return self.pairs(lambda l, y, x, c: (l, (y + dy) % self.ys, (x + dx) % self.xs, c))

    def swap(self):
        return self.pairs(lambda l, y, x, c: (l, y, x, CORES - 1 - c))

    def plane_offsets(self):
        return [(dy, dx) for dy in range(self.ys) for dx in range(self.xs) if dy or dx]

    def line_maps(self):
        maps = []
        for step in range(1, (self.lines + 1) // 2):
            maps.append({i: (i + step) % self.lines for i in range(self.lines)})
        if self.lines % 2 == 0:
            half = self.lines // 2
            maps.append({(i if i % 2 == 0 else i + half): (i + half if i % 2 == 0 else i) for i in range(half)})
        return maps

    def line_move(self, line_map):
        return self.pairs(lambda l, y, x, c: (line_map[l], y, x, c) if l in line_map else None)

    def line_return(self, line_map):
        back = {b: a for a, b in line_map.items()}
        free = [i for i in range(self.lines) if i not in line_map]
        back.update(zip([i for i in range(self.lines) if i not in back], free))
        return self.line_move(back)


def backward(pairs):
    return [(b, a) for a, b in pairs]


def pack_body(pieces, chunk, emb_hbm, order_hbm, out_ref, *refs):
    piece_refs, (emb_ref, order_ref, sems) = refs[: len(pieces)], refs[len(pieces) :]
    n, width = emb_ref.shape
    order_copy = pltpu.make_async_copy(order_hbm, order_ref, sems.at[0])
    order_copy.start()
    copies = []
    for k in range(n // chunk):
        rows = pl.ds(k * chunk, chunk)
        copies.append(pltpu.make_async_copy(emb_hbm.at[rows, :], emb_ref.at[rows, :], sems.at[k + 1]))
        copies[-1].start()
    out_ref[n:, :] = jnp.zeros((PAD, width), jnp.bfloat16)
    order_copy.wait()
    code = order_ref[...].reshape(1, n) + 1
    high = (code >> 8).astype(jnp.float32)
    low = (code & 255).astype(jnp.float32)
    line = lax.broadcasted_iota(jnp.int32, (PAD, n), 0)
    tail = jnp.where(line == 0, high, jnp.where(line == 1, low, 0.0))
    out_ref[n:, :n] = tail.astype(jnp.bfloat16)
    for k in range(n // chunk):
        copies[k].wait()
        rows = slice(k * chunk, (k + 1) * chunk)
        floats = emb_ref[rows, :].astype(jnp.float32)
        scale = lax.rsqrt(jnp.sum(floats * floats, axis=1, keepdims=True) + 1e-06)
        out_ref[rows, :] = (floats * scale).astype(jnp.bfloat16)
    for (start, rows), ref in zip(pieces, piece_refs):
        cut(out_ref, start, rows, ref)


def pack(embeddings, doc_order, pieces):
    n, width = embeddings.shape
    chunk = 128 if n % 128 == 0 else n
    call = pl.pallas_call(
        functools.partial(pack_body, pieces, chunk),
        in_specs=[pl.BlockSpec(memory_space=pltpu.HBM)] * 2,
        out_shape=[pltpu.VMEM((rows + PAD, width), jnp.bfloat16) for rows in (n, *(rows for _, rows in pieces))],
        scratch_shapes=[
            pltpu.VMEM((n, width), jnp.bfloat16),
            pltpu.VMEM((n,), jnp.int32),
            pltpu.SemaphoreType.DMA((n // chunk + 1,)),
        ],
        compiler_params=pltpu.CompilerParams(vmem_limit_bytes=VMEM_GRANT),
        name="pack",
    )
    return call(*(pltpu.with_memory_space_constraint(v, pltpu.HBM) for v in (embeddings, doc_order)))


def cut(ref, start, rows, out_ref):
    n = ref.shape[0] - PAD
    out_ref[:rows, :] = ref[start : start + rows, :]
    out_ref[rows:, :] = jnp.zeros((PAD, ref.shape[1]), jnp.bfloat16)
    out_ref[rows:, :rows] = ref[n:, start : start + rows]


def piece_body(start, rows, ref, out_ref):
    cut(ref, start, rows, out_ref)


def piece(block, start, rows):
    return pl.pallas_call(
        functools.partial(piece_body, start, rows),
        out_shape=pltpu.VMEM((rows + PAD, block.shape[1]), jnp.bfloat16),
        compiler_params=pltpu.CompilerParams(vmem_limit_bytes=VMEM_GRANT),
        name="piece",
    )(*in_vmem([block]))


def lane_orders(ref):
    n = ref.shape[0] - PAD
    tail = ref[n:, :n].astype(jnp.float32)
    order = tail[0:1] * 256.0 + tail[1:2]
    return jnp.where(order == 0.0, FAR, order)


def match_body(plan, chips, known, *refs):
    at = 0

    def take(count):
        nonlocal at
        at += count
        return refs[at - count : at]

    side_cols = sum(chips)
    rows, ours, twins = take(len(plan)), take(side_cols), take(side_cols)
    row_in, col_in = list(take(sum(p[2] for p in plan))), take(2 * known.count(0))
    row_out, col_out = take(1 + max(p[3] for p in plan)), take(2)
    (col_acc,) = take(1)
    lanes = 128
    firsts = [sum(chips[:k]) for k in range(len(chips) + 1)]
    fresh = set()
    for r, (meets, counted, has_known, out, first_lane) in enumerate(plan):
        n = rows[r].shape[0] - PAD
        own_orders = lane_orders(rows[r])
        own_order = jnp.broadcast_to(own_orders, (lanes, n)).T[:, 0:1]
        best = jnp.full((n, lanes), -1.0, jnp.float32)
        for chip in meets:
            blocks = [side[c] for side in (ours, twins) for c in range(firsts[chip], firsts[chip + 1])]
            units = jnp.concatenate([ref[: ref.shape[0] - PAD, :] for ref in blocks], axis=0)
            orders = jnp.concatenate([lane_orders(ref) for ref in blocks], axis=1)
            score = lax.dot_general(
                rows[r][:n, :], units, (((1,), (1,)), ((), ())), preferred_element_type=jnp.float32
            )
            for k in range(0, units.shape[0], lanes):
                part = score[:, k : k + lanes]
                earlier = orders[:, k : k + lanes] < own_order
                best = jnp.maximum(best, jnp.where(earlier, part, -1.0))
                if counted:
                    other = jnp.max(jnp.where(earlier, -1.0, part).reshape(n // 8, 8, lanes), axis=0)
                    if chip in fresh:
                        other = jnp.maximum(col_acc[chip, :, k : k + lanes], other)
                    col_acc[chip, :, k : k + lanes] = other
            if counted:
                fresh.add(chip)
        value = jnp.where(own_orders == FAR, -1.0, jnp.max(best.T, axis=0, keepdims=True))
        if has_known:
            value = jnp.maximum(value, row_in.pop(0)[...])
        row_out[out][0:1, first_lane : first_lane + n] = value
    for side in range(2):
        before = [col_in[side * known.count(0) + i][k : k + 1, :] for i, k in zip(group_index(known), known)]
        n = col_out[side].shape[1]
        for chip in range(len(chips)):
            value = jnp.max(col_acc[chip, :, side * n : (side + 1) * n], axis=0, keepdims=True)
            if chip < len(before):
                value = jnp.maximum(value, before[chip])
            col_out[side][chip : chip + 1, :] = value


def group_index(known):
    groups = []
    for k in known:
        groups.append((groups[-1] if groups else -1) + (k == 0))
    return groups


def in_vmem(values):
    return [pltpu.with_memory_space_constraint(v, pltpu.VMEM) for v in values]


def match(rows, chips, col_in=()):
    ours = [block for mine, _ in chips for block in mine]
    twins = [block for _, other in chips for block in other]
    width = rows[0][0].shape[1]
    n = sum(block.shape[0] - PAD for block in chips[0][0])
    sizes = [row[0].shape[0] - PAD for row in rows]
    plan = [(tuple(meets), counted, value is not None, out, lane) for _, meets, counted, value, out, lane in rows]
    totals = [max(p[4] + size for p, size in zip(plan, sizes) if p[3] == k) for k in range(1 + max(p[3] for p in plan))]
    known = [k for pair in col_in for k in range(pair[0].shape[0])]
    before = [pair[0] for pair in col_in] + [pair[1] for pair in col_in]
    block = pltpu.VMEM((len(chips), n), jnp.float32)
    call = pl.pallas_call(
        functools.partial(match_body, plan, [len(mine) for mine, _ in chips], known),
        out_shape=[pltpu.VMEM((1, total), jnp.float32) for total in totals] + [block, block],
        scratch_shapes=[pltpu.VMEM((len(chips), 8, 2 * n), jnp.float32)],
        cost_estimate=pl.CostEstimate(
            flops=4 * sum(size * len(p[0]) for p, size in zip(plan, sizes)) * n * width,
            bytes_accessed=2 * (sum(sizes) + 2 * len(chips) * n) * width,
            transcendentals=0,
        ),
        compiler_params=pltpu.CompilerParams(vmem_limit_bytes=VMEM_GRANT),
    )
    values = [row[3] for row in rows if row[3] is not None]
    outs = call(*in_vmem([*(row[0] for row in rows), *ours, *twins, *values, *before]))
    return outs[: len(totals)], tuple(outs[len(totals) :])


def merge_body(ours_ref, theirs_ref, *out_refs):
    value = jnp.maximum(ours_ref[...], theirs_ref[...])
    for k, ref in enumerate(out_refs):
        ref[...] = value[k : k + 1]


def merge(ours, theirs):
    count, n = ours.shape
    return pl.pallas_call(
        merge_body,
        out_shape=[pltpu.VMEM((1, n), jnp.float32)] * count,
        compiler_params=pltpu.CompilerParams(vmem_limit_bytes=VMEM_GRANT),
        name="merge",
    )(*in_vmem([ours, theirs]))


def solution(mesh):
    layout = Layout(mesh)
    maps = layout.line_maps()
    offsets = layout.plane_offsets()

    def send(value, pairs):
        return lax.ppermute(value, AXES, pairs)

    def nearest(embeddings, doc_order):
        n = embeddings.shape[0]
        last = min(n, 128)
        pieces = ((0, n - last), (n - last, last)) if n > last else ((0, n),)
        swap = layout.swap()

        own, *parts = pack(embeddings, doc_order, pieces)
        line = [send(own, layout.line_move(m)) for m in maps[:-1]]
        plane = [send(own, layout.plane_move(*d)) for d in offsets[:-1]]
        half = [send(part, layout.line_move(maps[-1])) for part in parts]

        dy, dx = offsets[-1]
        routes = [((0, dx), (dy, 0)), ((dy, 0), (0, dx))]
        corner = []
        for k, (start, rows) in enumerate(pieces):
            have, move = routes[k % 2]
            block = piece(plane[offsets.index(have)], start, rows)
            corner.append(send(block, layout.plane_move(*move)))
        near_chips = [([block], [send(block, swap)]) for block in [own, *plane]]
        far_chip = (corner, [send(block, swap) for block in corner])

        every = range(len(near_chips))
        far = len(near_chips)
        first = [own, *line]
        rows = [(block, every, k > 0, None, k, 0) for k, block in enumerate(first)]
        best, cols = match(rows, near_chips)
        side, cols = match([(block, every, True, None, k, 0) for k, block in enumerate(half[:-1])], near_chips, [cols])
        rows = [(block, [far], k > 0, best[k], k, 0) for k, block in enumerate(first)]
        rows += [(block, [far], True, side[k], len(first), pieces[k][0]) for k, block in enumerate(half[:-1])]
        rows.append((half[-1], [far, *every], True, None, len(first), pieces[-1][0]))
        best, (ours, theirs) = match(rows, [*near_chips, far_chip], [cols])

        theirs = send(theirs, swap)
        back = [best[0]]
        for value, m in zip(best[1:], maps):
            back.append(send(value, layout.line_return(m)))
        own_best, *others = merge(ours, theirs)
        back.append(own_best)
        for value, d in zip(others, offsets):
            back.append(send(value, backward(layout.plane_move(*d))))
        best = functools.reduce(jnp.maximum, back)
        return jnp.maximum(best, -1.0).reshape(doc_order.shape)

    return jax.shard_map(
        nearest,
        mesh=mesh,
        in_specs=(P(AXES, None), P(AXES)),
        out_specs=P(AXES),
        check_vma=False,
    )
```

```python
import functools

import jax
import jax.numpy as jnp
from jax import lax
from jax.experimental import pallas as pl
from jax.experimental.pallas import tpu as pltpu
from jax.sharding import PartitionSpec as P

AXES = ("row", "col")
CORES = 2
PAD = 16
FAR = 1.0e9
VMEM_GRANT = 16 << 20


class Layout:
    def __init__(self, mesh):
        rows, cols = mesh.shape["row"], mesh.shape["col"]
        self.xs = cols // CORES
        self.ys = self.xs if rows % self.xs == 0 else 1
        self.lines = rows // self.ys

    def index(self, line, y, x, core):
        return ((line * self.ys + y) * self.xs + x) * CORES + core

    def pairs(self, target):
        found = []
        for line in range(self.lines):
            for y in range(self.ys):
                for x in range(self.xs):
                    for core in range(CORES):
                        to = target(line, y, x, core)
                        if to is not None:
                            found.append((self.index(line, y, x, core), self.index(*to)))
        return found

    def plane_move(self, dy, dx):
        return self.pairs(lambda l, y, x, c: (l, (y + dy) % self.ys, (x + dx) % self.xs, c))

    def swap(self):
        return self.pairs(lambda l, y, x, c: (l, y, x, CORES - 1 - c))

    def plane_offsets(self):
        return [(dy, dx) for dy in range(self.ys) for dx in range(self.xs) if dy or dx]

    def line_maps(self):
        maps = []
        for step in range(1, (self.lines + 1) // 2):
            maps.append({i: (i + step) % self.lines for i in range(self.lines)})
        if self.lines % 2 == 0:
            half = self.lines // 2
            maps.append({(i if i % 2 == 0 else i + half): (i + half if i % 2 == 0 else i) for i in range(half)})
        return maps

    def line_move(self, line_map):
        return self.pairs(lambda l, y, x, c: (line_map[l], y, x, c) if l in line_map else None)

    def line_hops(self):
        return [{(b - 1) % self.lines: b for b in m.values()} for m in self.line_maps()]

    def line_return(self, line_map):
        back = {b: a for a, b in line_map.items()}
        free = [i for i in range(self.lines) if i not in line_map]
        back.update(zip([i for i in range(self.lines) if i not in back], free))
        return self.line_move(back)


def backward(pairs):
    return [(b, a) for a, b in pairs]


def pack_body(pieces, chunk, emb_hbm, order_hbm, out_ref, *refs):
    piece_refs, (emb_ref, order_ref, sems) = refs[: len(pieces)], refs[len(pieces) :]
    n, width = emb_ref.shape
    order_copy = pltpu.make_async_copy(order_hbm, order_ref, sems.at[0])
    order_copy.start()
    copies = []
    for k in range(n // chunk):
        rows = pl.ds(k * chunk, chunk)
        copies.append(pltpu.make_async_copy(emb_hbm.at[rows, :], emb_ref.at[rows, :], sems.at[k + 1]))
        copies[-1].start()
    out_ref[n:, :] = jnp.zeros((PAD, width), jnp.bfloat16)
    order_copy.wait()
    code = order_ref[...].reshape(1, n) + 1
    high = (code >> 8).astype(jnp.float32)
    low = (code & 255).astype(jnp.float32)
    line = lax.broadcasted_iota(jnp.int32, (PAD, n), 0)
    tail = jnp.where(line == 0, high, jnp.where(line == 1, low, 0.0))
    out_ref[n:, :n] = tail.astype(jnp.bfloat16)
    for k in range(n // chunk):
        copies[k].wait()
        rows = slice(k * chunk, (k + 1) * chunk)
        floats = emb_ref[rows, :].astype(jnp.float32)
        scale = lax.rsqrt(jnp.sum(floats * floats, axis=1, keepdims=True) + 1e-06)
        out_ref[rows, :] = (floats * scale).astype(jnp.bfloat16)
    for (start, rows), ref in zip(pieces, piece_refs):
        cut(out_ref, start, rows, ref)


def pack(embeddings, doc_order, pieces):
    n, width = embeddings.shape
    chunk = 128 if n % 128 == 0 else n
    call = pl.pallas_call(
        functools.partial(pack_body, pieces, chunk),
        in_specs=[pl.BlockSpec(memory_space=pltpu.HBM)] * 2,
        out_shape=[pltpu.VMEM((rows + PAD, width), jnp.bfloat16) for rows in (n, *(rows for _, rows in pieces))],
        scratch_shapes=[
            pltpu.VMEM((n, width), jnp.bfloat16),
            pltpu.VMEM((n,), jnp.int32),
            pltpu.SemaphoreType.DMA((n // chunk + 1,)),
        ],
        compiler_params=pltpu.CompilerParams(vmem_limit_bytes=VMEM_GRANT),
        name="pack",
    )
    return call(*(pltpu.with_memory_space_constraint(v, pltpu.HBM) for v in (embeddings, doc_order)))


def cut(ref, start, rows, out_ref):
    n = ref.shape[0] - PAD
    out_ref[:rows, :] = ref[start : start + rows, :]
    out_ref[rows:, :] = jnp.zeros((PAD, ref.shape[1]), jnp.bfloat16)
    out_ref[rows:, :rows] = ref[n:, start : start + rows]


def piece_body(start, rows, ref, out_ref):
    cut(ref, start, rows, out_ref)


def piece(block, start, rows):
    return pl.pallas_call(
        functools.partial(piece_body, start, rows),
        out_shape=pltpu.VMEM((rows + PAD, block.shape[1]), jnp.bfloat16),
        compiler_params=pltpu.CompilerParams(vmem_limit_bytes=VMEM_GRANT),
        name="piece",
    )(*in_vmem([block]))


def lane_orders(ref):
    n = ref.shape[0] - PAD
    tail = ref[n:, :n].astype(jnp.float32)
    order = tail[0:1] * 256.0 + tail[1:2]
    return jnp.where(order == 0.0, FAR, order)


def match_body(plan, chips, known, *refs):
    at = 0

    def take(count):
        nonlocal at
        at += count
        return refs[at - count : at]

    side_cols = sum(chips)
    rows, ours, twins = take(len(plan)), take(side_cols), take(side_cols)
    row_in, col_in = list(take(sum(p[2] for p in plan))), take(2 * known.count(0))
    row_out, col_out = take(1 + max(p[3] for p in plan)), take(2)
    (col_acc,) = take(1)
    lanes = 128
    firsts = [sum(chips[:k]) for k in range(len(chips) + 1)]
    fresh = set()
    for r, (meets, counted, has_known, out, first_lane) in enumerate(plan):
        n = rows[r].shape[0] - PAD
        own_orders = lane_orders(rows[r])
        own_order = jnp.broadcast_to(own_orders, (lanes, n)).T[:, 0:1]
        best = jnp.full((n, lanes), -1.0, jnp.float32)
        for chip in meets:
            blocks = [side[c] for side in (ours, twins) for c in range(firsts[chip], firsts[chip + 1])]
            units = jnp.concatenate([ref[: ref.shape[0] - PAD, :] for ref in blocks], axis=0)
            orders = jnp.concatenate([lane_orders(ref) for ref in blocks], axis=1)
            score = lax.dot_general(
                rows[r][:n, :], units, (((1,), (1,)), ((), ())), preferred_element_type=jnp.float32
            )
            for k in range(0, units.shape[0], lanes):
                part = score[:, k : k + lanes]
                earlier = orders[:, k : k + lanes] < own_order
                best = jnp.maximum(best, jnp.where(earlier, part, -1.0))
                if counted:
                    other = jnp.max(jnp.where(earlier, -1.0, part).reshape(n // 8, 8, lanes), axis=0)
                    if chip in fresh:
                        other = jnp.maximum(col_acc[chip, :, k : k + lanes], other)
                    col_acc[chip, :, k : k + lanes] = other
            if counted:
                fresh.add(chip)
        value = jnp.where(own_orders == FAR, -1.0, jnp.max(best.T, axis=0, keepdims=True))
        if has_known:
            value = jnp.maximum(value, row_in.pop(0)[0:1, first_lane : first_lane + n])
        row_out[out][0:1, first_lane : first_lane + n] = value
    for side in range(2):
        before = [col_in[side * known.count(0) + i][k : k + 1, :] for i, k in zip(group_index(known), known)]
        n = col_out[side].shape[1]
        for chip in range(len(chips)):
            value = jnp.max(col_acc[chip, :, side * n : (side + 1) * n], axis=0, keepdims=True)
            if chip < len(before):
                value = jnp.maximum(value, before[chip])
            col_out[side][chip : chip + 1, :] = value


def group_index(known):
    groups = []
    for k in known:
        groups.append((groups[-1] if groups else -1) + (k == 0))
    return groups


def in_vmem(values):
    return [pltpu.with_memory_space_constraint(v, pltpu.VMEM) for v in values]


def match(rows, chips, col_in=()):
    ours = [block for mine, _ in chips for block in mine]
    twins = [block for _, other in chips for block in other]
    width = rows[0][0].shape[1]
    n = sum(block.shape[0] - PAD for block in chips[0][0])
    sizes = [row[0].shape[0] - PAD for row in rows]
    plan = [(tuple(meets), counted, value is not None, out, lane) for _, meets, counted, value, out, lane in rows]
    totals = [max(p[4] + size for p, size in zip(plan, sizes) if p[3] == k) for k in range(1 + max(p[3] for p in plan))]
    known = [k for pair in col_in for k in range(pair[0].shape[0])]
    before = [pair[0] for pair in col_in] + [pair[1] for pair in col_in]
    block = pltpu.VMEM((len(chips), n), jnp.float32)
    call = pl.pallas_call(
        functools.partial(match_body, plan, [len(mine) for mine, _ in chips], known),
        out_shape=[pltpu.VMEM((1, total), jnp.float32) for total in totals] + [block, block],
        scratch_shapes=[pltpu.VMEM((len(chips), 8, 2 * n), jnp.float32)],
        cost_estimate=pl.CostEstimate(
            flops=4 * sum(size * len(p[0]) for p, size in zip(plan, sizes)) * n * width,
            bytes_accessed=2 * (sum(sizes) + 2 * len(chips) * n) * width,
            transcendentals=0,
        ),
        compiler_params=pltpu.CompilerParams(vmem_limit_bytes=VMEM_GRANT),
    )
    values = [row[3] for row in rows if row[3] is not None]
    outs = call(*in_vmem([*(row[0] for row in rows), *ours, *twins, *values, *before]))
    return outs[: len(totals)], tuple(outs[len(totals) :])


def merge_body(ours_ref, theirs_ref, *out_refs):
    value = jnp.maximum(ours_ref[...], theirs_ref[...])
    for k, ref in enumerate(out_refs):
        ref[...] = value[k : k + 1]


def merge(ours, theirs):
    count, n = ours.shape
    return pl.pallas_call(
        merge_body,
        out_shape=[pltpu.VMEM((1, n), jnp.float32)] * count,
        compiler_params=pltpu.CompilerParams(vmem_limit_bytes=VMEM_GRANT),
        name="merge",
    )(*in_vmem([ours, theirs]))


def solution(mesh):
    layout = Layout(mesh)
    maps = layout.line_maps()
    offsets = layout.plane_offsets()

    def send(value, pairs):
        return lax.ppermute(value, AXES, pairs)

    def nearest(embeddings, doc_order):
        n = embeddings.shape[0]
        last = min(n, 128)
        pieces = ((0, n - last), (n - last, last)) if n > last else ((0, n),)
        swap = layout.swap()

        own, *parts = pack(embeddings, doc_order, pieces)
        line = []
        for hop in layout.line_hops():
            parts = [send(part, layout.line_move(hop)) for part in parts]
            line.append(parts)
        plane = [send(own, layout.plane_move(*d)) for d in offsets[:-1]]

        dy, dx = offsets[-1]
        routes = [((0, dx), (dy, 0)), ((dy, 0), (0, dx))]
        corner = []
        for k, (start, rows) in enumerate(pieces):
            have, move = routes[k % 2]
            block = piece(plane[offsets.index(have)], start, rows)
            corner.append(send(block, layout.plane_move(*move)))
        near_chips = [([block], [send(block, swap)]) for block in [own, *plane]]
        far_chip = (corner, [send(block, swap) for block in corner])

        every = range(len(near_chips))
        far = len(near_chips)
        lanes = [start for start, _ in pieces]
        first = [(own, False, 0, 0)]
        first += [(block, True, k + 1, lane) for k, step in enumerate(line[:-1]) for block, lane in zip(step, lanes)]
        half = [(block, True, len(line), lane) for block, lane in zip(line[-1], lanes)]
        best, cols = match([(r[0], every, r[1], None, *r[2:]) for r in first], near_chips)
        side, cols = match([(r[0], every, True, None, 0, r[3]) for r in half[:-1]], near_chips, [cols])
        known = [*best, *side]
        rows = [(r[0], [far], r[1], known[r[2]], *r[2:]) for r in first + half[:-1]]
        rows.append((half[-1][0], [far, *every], True, None, *half[-1][2:]))
        best, (ours, theirs) = match(rows, [*near_chips, far_chip], [cols])

        theirs = send(theirs, swap)
        back = [best[0]]
        for value, m in zip(best[1:], maps):
            back.append(send(value, layout.line_return(m)))
        own_best, *others = merge(ours, theirs)
        back.append(own_best)
        for value, d in zip(others, offsets):
            back.append(send(value, backward(layout.plane_move(*d))))
        best = functools.reduce(jnp.maximum, back)
        return jnp.maximum(best, -1.0).reshape(doc_order.shape)

    return jax.shard_map(
        nearest,
        mesh=mesh,
        in_specs=(P(AXES, None), P(AXES)),
        out_specs=P(AXES),
        check_vma=False,
    )
```

```python
import functools

import jax
import jax.numpy as jnp
from jax import lax
from jax.experimental import pallas as pl
from jax.experimental.pallas import tpu as pltpu
from jax.sharding import PartitionSpec as P

AXES = ("row", "col")
CORES = 2
PAD = 16
FAR = 1.0e9
VMEM_GRANT = 16 << 20


class Layout:
    def __init__(self, mesh):
        rows, cols = mesh.shape["row"], mesh.shape["col"]
        self.xs = cols // CORES
        self.ys = self.xs if rows % self.xs == 0 else 1
        self.lines = rows // self.ys

    def index(self, line, y, x, core):
        return ((line * self.ys + y) * self.xs + x) * CORES + core

    def pairs(self, target):
        found = []
        for line in range(self.lines):
            for y in range(self.ys):
                for x in range(self.xs):
                    for core in range(CORES):
                        to = target(line, y, x, core)
                        if to is not None:
                            found.append((self.index(line, y, x, core), self.index(*to)))
        return found

    def plane_move(self, dy, dx):
        return self.pairs(lambda l, y, x, c: (l, (y + dy) % self.ys, (x + dx) % self.xs, c))

    def swap(self):
        return self.pairs(lambda l, y, x, c: (l, y, x, CORES - 1 - c))

    def plane_offsets(self):
        return [(dy, dx) for dy in range(self.ys) for dx in range(self.xs) if dy or dx]

    def line_maps(self):
        maps = []
        for step in range(1, (self.lines + 1) // 2):
            maps.append({i: (i + step) % self.lines for i in range(self.lines)})
        if self.lines % 2 == 0:
            half = self.lines // 2
            maps.append({(i if i % 2 == 0 else i + half): (i + half if i % 2 == 0 else i) for i in range(half)})
        return maps

    def line_move(self, line_map):
        return self.pairs(lambda l, y, x, c: (line_map[l], y, x, c) if l in line_map else None)

    def line_hops(self):
        return [{(b - 1) % self.lines: b for b in m.values()} for m in self.line_maps()]

    def line_return(self, line_map):
        back = {b: a for a, b in line_map.items()}
        free = [i for i in range(self.lines) if i not in line_map]
        back.update(zip([i for i in range(self.lines) if i not in back], free))
        return self.line_move(back)


def backward(pairs):
    return [(b, a) for a, b in pairs]


def pack_body(pieces, chunk, emb_hbm, order_hbm, out_ref, *refs):
    piece_refs, (emb_ref, order_ref, sems) = refs[: len(pieces)], refs[len(pieces) :]
    n, width = emb_ref.shape
    order_copy = pltpu.make_async_copy(order_hbm, order_ref, sems.at[0])
    order_copy.start()
    copies = []
    for k in range(n // chunk):
        rows = pl.ds(k * chunk, chunk)
        copies.append(pltpu.make_async_copy(emb_hbm.at[rows, :], emb_ref.at[rows, :], sems.at[k + 1]))
        copies[-1].start()
    out_ref[n:, :] = jnp.zeros((PAD, width), jnp.bfloat16)
    order_copy.wait()
    code = order_ref[...].reshape(1, n) + 1
    high = (code >> 8).astype(jnp.float32)
    low = (code & 255).astype(jnp.float32)
    line = lax.broadcasted_iota(jnp.int32, (PAD, n), 0)
    tail = jnp.where(line == 0, high, jnp.where(line == 1, low, 0.0))
    out_ref[n:, :n] = tail.astype(jnp.bfloat16)
    for k in range(n // chunk):
        copies[k].wait()
        rows = slice(k * chunk, (k + 1) * chunk)
        floats = emb_ref[rows, :].astype(jnp.float32)
        scale = lax.rsqrt(jnp.sum(floats * floats, axis=1, keepdims=True) + 1e-06)
        out_ref[rows, :] = (floats * scale).astype(jnp.bfloat16)
    for (start, rows), ref in zip(pieces, piece_refs):
        cut(out_ref, start, rows, ref)


def pack(embeddings, doc_order, pieces):
    n, width = embeddings.shape
    chunk = 128 if n % 128 == 0 else n
    call = pl.pallas_call(
        functools.partial(pack_body, pieces, chunk),
        in_specs=[pl.BlockSpec(memory_space=pltpu.HBM)] * 2,
        out_shape=[pltpu.VMEM((rows + PAD, width), jnp.bfloat16) for rows in (n, *(rows for _, rows in pieces))],
        scratch_shapes=[
            pltpu.VMEM((n, width), jnp.bfloat16),
            pltpu.VMEM((n,), jnp.int32),
            pltpu.SemaphoreType.DMA((n // chunk + 1,)),
        ],
        compiler_params=pltpu.CompilerParams(vmem_limit_bytes=VMEM_GRANT),
        name="pack",
    )
    return call(*(pltpu.with_memory_space_constraint(v, pltpu.HBM) for v in (embeddings, doc_order)))


def cut(ref, start, rows, out_ref):
    n = ref.shape[0] - PAD
    out_ref[:rows, :] = ref[start : start + rows, :]
    out_ref[rows:, :] = jnp.zeros((PAD, ref.shape[1]), jnp.bfloat16)
    out_ref[rows:, :rows] = ref[n:, start : start + rows]


def piece_body(start, rows, ref, out_ref):
    cut(ref, start, rows, out_ref)


def piece(block, start, rows):
    return pl.pallas_call(
        functools.partial(piece_body, start, rows),
        out_shape=pltpu.VMEM((rows + PAD, block.shape[1]), jnp.bfloat16),
        compiler_params=pltpu.CompilerParams(vmem_limit_bytes=VMEM_GRANT),
        name="piece",
    )(*in_vmem([block]))


def lane_orders(ref):
    n = ref.shape[0] - PAD
    tail = ref[n:, :n].astype(jnp.float32)
    order = tail[0:1] * 256.0 + tail[1:2]
    return jnp.where(order == 0.0, FAR, order)


def match_body(tasks, groups, initial, final, n_blocks, *refs):
    blocks, refs = refs[:n_blocks], refs[n_blocks:]
    before, refs = (None, refs) if initial else (refs[:3], refs[3:])
    row_out, col_out, col_acc = refs[:-3], refs[-3:-1], refs[-1]
    lanes = 128

    def result(row):
        return (row_out[row], 0) if final else (row_out[0], row)

    for side in range(2):
        if initial:
            col_out[side][...] = jnp.full(col_out[side].shape, -1.0, jnp.float32)
        else:
            col_out[side][...] = before[1 + side][...]
    for k in range(len(row_out)):
        if initial:
            row_out[k][...] = jnp.full(row_out[k].shape, -1.0, jnp.float32)
        else:
            row_out[k][...] = before[0][k : k + 1, :] if final else before[0][...]
    fresh = set()
    for block, row, lane, counted, meets in tasks:
        n = blocks[block].shape[0] - PAD
        own_orders = lane_orders(blocks[block])
        own_order = jnp.broadcast_to(own_orders, (lanes, n)).T[:, 0:1]
        best = jnp.full((n, lanes), -1.0, jnp.float32)
        for g in meets:
            cols = [blocks[col[0]] for col in groups[g]]
            units = jnp.concatenate([ref[: ref.shape[0] - PAD, :] for ref in cols], axis=0)
            orders = jnp.concatenate([lane_orders(ref) for ref in cols], axis=1)
            score = lax.dot_general(
                blocks[block][:n, :], units, (((1,), (1,)), ((), ())), preferred_element_type=jnp.float32
            )
            for k in range(0, units.shape[0], lanes):
                part = score[:, k : k + lanes]
                earlier = orders[:, k : k + lanes] < own_order
                best = jnp.maximum(best, jnp.where(earlier, part, -1.0))
                if counted:
                    other = jnp.max(jnp.where(earlier, -1.0, part).reshape(n // 8, 8, lanes), axis=0)
                    if g in fresh:
                        other = jnp.maximum(col_acc[g, :, k : k + lanes], other)
                    col_acc[g, :, k : k + lanes] = other
            if counted:
                fresh.add(g)
        value = jnp.where(own_orders == FAR, -1.0, jnp.max(best.T, axis=0, keepdims=True))
        ref, at = result(row)
        ref[at : at + 1, lane : lane + n] = jnp.maximum(ref[at : at + 1, lane : lane + n], value)
    for g in sorted(fresh):
        start = 0
        for col, side, chip, lane in groups[g]:
            n = blocks[col].shape[0] - PAD
            value = jnp.max(col_acc[g, :, start : start + n], axis=0, keepdims=True)
            ref = col_out[side]
            ref[chip : chip + 1, lane : lane + n] = jnp.maximum(ref[chip : chip + 1, lane : lane + n], value)
            start += n


def in_vmem(values):
    return [pltpu.with_memory_space_constraint(v, pltpu.VMEM) for v in values]


def match(state, tasks, shape, final=False):
    blocks, groups, plan = [], [], []

    def place(value, values):
        for k, known in enumerate(values):
            if known is value:
                return k
        values.append(value)
        return len(values) - 1

    for block, row, lane, counted, meets in tasks:
        found = []
        for group in meets:
            group = [(place(col, blocks), *where) for col, *where in group]
            if group not in groups:
                groups.append(group)
            found.append(groups.index(group))
        plan.append((place(block, blocks), row, lane, counted, found))
    rows, chips, n = shape
    width = blocks[0].shape[1]
    widest = max(sum(blocks[col[0]].shape[0] - PAD for col in group) for group in groups)
    pairs = sum(blocks[p[0]].shape[0] * blocks[col[0]].shape[0] for p in plan for g in p[4] for col in groups[g])
    best = [pltpu.VMEM((1, n), jnp.float32)] * rows if final else [pltpu.VMEM((rows, n), jnp.float32)]
    return pl.pallas_call(
        functools.partial(match_body, plan, groups, state is None, final, len(blocks)),
        out_shape=best + [pltpu.VMEM((chips, n), jnp.float32)] * 2,
        scratch_shapes=[pltpu.VMEM((len(groups), 8, widest), jnp.float32)],
        cost_estimate=pl.CostEstimate(flops=2 * pairs * width, bytes_accessed=2 * len(blocks) * n * width, transcendentals=0),
        compiler_params=pltpu.CompilerParams(vmem_limit_bytes=VMEM_GRANT),
    )(*in_vmem([*blocks, *(state or ())]))


def merge_body(ours_ref, theirs_ref, *out_refs):
    value = jnp.maximum(ours_ref[...], theirs_ref[...])
    for k, ref in enumerate(out_refs):
        ref[...] = value[k : k + 1]


def merge(ours, theirs):
    count, n = ours.shape
    return pl.pallas_call(
        merge_body,
        out_shape=[pltpu.VMEM((1, n), jnp.float32)] * count,
        compiler_params=pltpu.CompilerParams(vmem_limit_bytes=VMEM_GRANT),
        name="merge",
    )(*in_vmem([ours, theirs]))


def solution(mesh):
    layout = Layout(mesh)
    maps = layout.line_maps()
    offsets = layout.plane_offsets()

    def send(value, pairs):
        return lax.ppermute(value, AXES, pairs)

    def nearest(embeddings, doc_order):
        n = embeddings.shape[0]
        tile = 128
        pieces = ((0, tile), (tile, n - tile))
        corner_pieces = ((0, n - tile), (n - tile, tile))
        swap = layout.swap()

        own, *parts = pack(embeddings, doc_order, pieces)
        line = []
        for hop in layout.line_hops():
            parts = [send(part, layout.line_move(hop)) for part in parts]
            line.append(parts)
        plane = [send(own, layout.plane_move(*d)) for d in offsets[:-1]]

        dy, dx = offsets[-1]
        routes = [((0, dx), (dy, 0)), ((dy, 0), (0, dx))]
        corner = []
        for k, (start, rows) in enumerate(corner_pieces):
            have, move = routes[k % 2]
            block = piece(plane[offsets.index(have)], start, rows)
            corner.append(send(block, layout.plane_move(*move)))
        twins = [send(block, swap) for block in [own, *plane]]
        corner_twins = [send(block, swap) for block in corner]

        def by_two(blocks, side):
            cols = [(block, side, k + 1, 0) for k, block in enumerate(blocks)]
            return [cols[k : k + 2] for k in range(0, len(cols), 2)]

        far = len(offsets)
        own_cols = [[(own, 0, 0, 0), (twins[0], 1, 0, 0)]]
        plane_cols, twin_cols = by_two(plane, 0), by_two(twins[1:], 1)
        corner_cols = [[(block, 0, far, start) for block, (start, _) in zip(corner, corner_pieces)]]
        ctwin_cols = [[(block, 1, far, start) for block, (start, _) in zip(corner_twins, corner_pieces)]]

        lanes = [start for start, _ in pieces]
        mine = [(own, 0, 0, False)]
        early = [(block, k + 1, at, True) for k, step in enumerate(line[:-1]) for block, at in zip(step, lanes)]
        half_a, half_b = [(block, len(line), at, True) for block, at in zip(line[-1], lanes)]
        shape = (len(line) + 1, far + 1, n)
        state = match(None, [(*r, own_cols) for r in mine], shape)
        if early:
            state = match(state, [(*early[0], own_cols)], shape)
        rows = [(*r, own_cols * (k > 0) + plane_cols) for k, r in enumerate(early)]
        state = match(state, rows + [(*r, plane_cols) for r in mine], shape)
        state = match(state, [(*r, twin_cols) for r in mine + early], shape)
        near_cols = own_cols + plane_cols + twin_cols
        state = match(state, [(*half_a, near_cols)], shape)
        state = match(state, [(*r, corner_cols) for r in [*mine, *early, half_a]], shape)
        state = match(state, [(*half_b, near_cols + corner_cols)], shape)
        everyone = [*mine, *early, half_a, half_b]
        *best, ours, theirs = match(state, [(*r, ctwin_cols) for r in everyone], shape, True)

        theirs = send(theirs, swap)
        back = [best[0]]
        for value, m in zip(best[1:], maps):
            back.append(send(value, layout.line_return(m)))
        own_best, *others = merge(ours, theirs)
        back.append(own_best)
        for value, d in zip(others, offsets):
            back.append(send(value, backward(layout.plane_move(*d))))
        best = functools.reduce(jnp.maximum, back)
        return jnp.maximum(best, -1.0).reshape(doc_order.shape)

    return jax.shard_map(
        nearest,
        mesh=mesh,
        in_specs=(P(AXES, None), P(AXES)),
        out_specs=P(AXES),
        check_vma=False,
    )
```

```python
import functools

import jax
import jax.numpy as jnp
from jax import lax
from jax.experimental import pallas as pl
from jax.experimental.pallas import tpu as pltpu
from jax.sharding import PartitionSpec as P

AXES = ("row", "col")
CORES = 2
PAD = 16
FAR = 1.0e9
VMEM_GRANT = 16 << 20


class Layout:
    def __init__(self, mesh):
        rows, cols = mesh.shape["row"], mesh.shape["col"]
        self.xs = cols // CORES
        self.ys = self.xs if rows % self.xs == 0 else 1
        self.lines = rows // self.ys

    def index(self, line, y, x, core):
        return ((line * self.ys + y) * self.xs + x) * CORES + core

    def pairs(self, target):
        found = []
        for line in range(self.lines):
            for y in range(self.ys):
                for x in range(self.xs):
                    for core in range(CORES):
                        to = target(line, y, x, core)
                        if to is not None:
                            found.append((self.index(line, y, x, core), self.index(*to)))
        return found

    def plane_move(self, dy, dx):
        return self.pairs(lambda l, y, x, c: (l, (y + dy) % self.ys, (x + dx) % self.xs, c))

    def swap(self):
        return self.pairs(lambda l, y, x, c: (l, y, x, CORES - 1 - c))

    def plane_offsets(self):
        return [(dy, dx) for dy in range(self.ys) for dx in range(self.xs) if dy or dx]

    def line_maps(self):
        maps = []
        for step in range(1, (self.lines + 1) // 2):
            maps.append({i: (i + step) % self.lines for i in range(self.lines)})
        if self.lines % 2 == 0:
            half = self.lines // 2
            maps.append({(i if i % 2 == 0 else i + half): (i + half if i % 2 == 0 else i) for i in range(half)})
        return maps

    def line_move(self, line_map):
        return self.pairs(lambda l, y, x, c: (line_map[l], y, x, c) if l in line_map else None)

    def line_hops(self):
        return [{(b - 1) % self.lines: b for b in m.values()} for m in self.line_maps()]

    def line_return(self, line_map):
        back = {b: a for a, b in line_map.items()}
        free = [i for i in range(self.lines) if i not in line_map]
        back.update(zip([i for i in range(self.lines) if i not in back], free))
        return self.line_move(back)


def backward(pairs):
    return [(b, a) for a, b in pairs]


def pack_body(pieces, chunk, emb_hbm, order_hbm, out_ref, *refs):
    piece_refs, (emb_ref, order_ref, sems) = refs[: len(pieces)], refs[len(pieces) :]
    n, width = emb_ref.shape
    order_copy = pltpu.make_async_copy(order_hbm, order_ref, sems.at[0])
    order_copy.start()
    copies = []
    for k in range(n // chunk):
        rows = pl.ds(k * chunk, chunk)
        copies.append(pltpu.make_async_copy(emb_hbm.at[rows, :], emb_ref.at[rows, :], sems.at[k + 1]))
        copies[-1].start()
    out_ref[n:, :] = jnp.zeros((PAD, width), jnp.bfloat16)
    order_copy.wait()
    code = order_ref[...].reshape(1, n) + 1
    high = (code >> 8).astype(jnp.float32)
    low = (code & 255).astype(jnp.float32)
    line = lax.broadcasted_iota(jnp.int32, (PAD, n), 0)
    tail = jnp.where(line == 0, high, jnp.where(line == 1, low, 0.0))
    out_ref[n:, :n] = tail.astype(jnp.bfloat16)
    for k in range(n // chunk):
        copies[k].wait()
        rows = slice(k * chunk, (k + 1) * chunk)
        floats = emb_ref[rows, :].astype(jnp.float32)
        scale = lax.rsqrt(jnp.sum(floats * floats, axis=1, keepdims=True) + 1e-06)
        out_ref[rows, :] = (floats * scale).astype(jnp.bfloat16)
    for (start, rows), ref in zip(pieces, piece_refs):
        cut(out_ref, start, rows, ref)


def pack(embeddings, doc_order, pieces):
    n, width = embeddings.shape
    chunk = 128 if n % 128 == 0 else n
    call = pl.pallas_call(
        functools.partial(pack_body, pieces, chunk),
        in_specs=[pl.BlockSpec(memory_space=pltpu.HBM)] * 2,
        out_shape=[pltpu.VMEM((rows + PAD, width), jnp.bfloat16) for rows in (n, *(rows for _, rows in pieces))],
        scratch_shapes=[
            pltpu.VMEM((n, width), jnp.bfloat16),
            pltpu.VMEM((n,), jnp.int32),
            pltpu.SemaphoreType.DMA((n // chunk + 1,)),
        ],
        compiler_params=pltpu.CompilerParams(vmem_limit_bytes=VMEM_GRANT),
        name="pack",
    )
    return call(*(pltpu.with_memory_space_constraint(v, pltpu.HBM) for v in (embeddings, doc_order)))


def cut(ref, start, rows, out_ref):
    n = ref.shape[0] - PAD
    out_ref[:rows, :] = ref[start : start + rows, :]
    out_ref[rows:, :] = jnp.zeros((PAD, ref.shape[1]), jnp.bfloat16)
    out_ref[rows:, :rows] = ref[n:, start : start + rows]


def piece_body(start, rows, ref, out_ref):
    cut(ref, start, rows, out_ref)


def piece(block, start, rows):
    return pl.pallas_call(
        functools.partial(piece_body, start, rows),
        out_shape=pltpu.VMEM((rows + PAD, block.shape[1]), jnp.bfloat16),
        compiler_params=pltpu.CompilerParams(vmem_limit_bytes=VMEM_GRANT),
        name="piece",
    )(*in_vmem([block]))


def lane_orders(ref):
    n = ref.shape[0] - PAD
    tail = ref[n:, :n].astype(jnp.float32)
    order = tail[0:1] * 256.0 + tail[1:2]
    return jnp.where(order == 0.0, FAR, order)


def match_body(tasks, groups, n_blocks, n_rows, initial, *refs):
    blocks, refs = refs[:n_blocks], refs[n_blocks:]
    before, after, col_acc = refs[: len(refs) - n_rows - 3], refs[-n_rows - 3 : -1], refs[-1]
    row_out, col_out = after[:n_rows], after[n_rows:]
    lanes = 128
    for k, ref in enumerate(after):
        ref[...] = jnp.full(ref.shape, -1.0, jnp.float32) if initial else before[k][...]

    def units_of(numbers):
        parts = [blocks[k][: blocks[k].shape[0] - PAD, :] for k in numbers]
        return parts[0] if len(parts) == 1 else jnp.concatenate(parts, axis=0)

    fresh = set()
    for rows, meets in tasks:
        row_units = units_of([row[0] for row in rows])
        sizes = [blocks[row[0]].shape[0] - PAD for row in rows]
        row_orders = [lane_orders(blocks[row[0]]) for row in rows]
        columns = [jnp.broadcast_to(orders, (lanes, n)).T[:, 0:1] for orders, n in zip(row_orders, sizes)]
        best = [jnp.full((n, lanes), -1.0, jnp.float32) for n in sizes]
        for g in meets:
            numbers = [col[0] for col in groups[g]]
            orders = jnp.concatenate([lane_orders(blocks[k]) for k in numbers], axis=1)
            score = lax.dot_general(
                row_units, units_of(numbers), (((1,), (1,)), ((), ())), preferred_element_type=jnp.float32
            )
            for k in range(0, score.shape[1], lanes):
                first = 0
                kept = [col_acc[g, :, k : k + lanes]] if g in fresh else []
                for r, (_, _, _, counted) in enumerate(rows):
                    n = sizes[r]
                    part = score[first : first + n, k : k + lanes]
                    earlier = orders[:, k : k + lanes] < columns[r]
                    best[r] = jnp.maximum(best[r], jnp.where(earlier, part, -1.0))
                    if counted:
                        kept.append(jnp.max(jnp.where(earlier, -1.0, part).reshape(n // 8, 8, lanes), axis=0))
                    first += n
                if any(row[3] for row in rows):
                    col_acc[g, :, k : k + lanes] = functools.reduce(jnp.maximum, kept)
            if any(row[3] for row in rows):
                fresh.add(g)
        for r, (_, row, lane, _) in enumerate(rows):
            value = jnp.where(row_orders[r] == FAR, -1.0, jnp.max(best[r].T, axis=0, keepdims=True))
            at = slice(lane, lane + sizes[r])
            row_out[row][:, at] = jnp.maximum(row_out[row][:, at], value)
    for g in sorted(fresh):
        start = 0
        for col, side, chip, lane in groups[g]:
            n = blocks[col].shape[0] - PAD
            value = jnp.max(col_acc[g, :, start : start + n], axis=0, keepdims=True)
            ref = col_out[side]
            ref[chip : chip + 1, lane : lane + n] = jnp.maximum(ref[chip : chip + 1, lane : lane + n], value)
            start += n


def in_vmem(values):
    return [pltpu.with_memory_space_constraint(v, pltpu.VMEM) for v in values]


def match(state, tasks, shape):
    blocks, groups, plan = [], [], []

    def place(value):
        for k, known in enumerate(blocks):
            if known is value:
                return k
        blocks.append(value)
        return len(blocks) - 1

    for rows, meets in tasks:
        found = []
        for group in meets:
            group = [(place(col), *where) for col, *where in group]
            if group not in groups:
                groups.append(group)
            found.append(groups.index(group))
        plan.append(([(place(row), *where) for row, *where in rows], found))
    rows, chips, n = shape
    width = blocks[0].shape[1]
    widest = max(sum(blocks[col[0]].shape[0] - PAD for col in group) for group in groups)
    pairs = sum(blocks[r[0]].shape[0] * blocks[col[0]].shape[0] for p in plan for r in p[0] for g in p[1] for col in groups[g])
    return pl.pallas_call(
        functools.partial(match_body, plan, groups, len(blocks), rows, state is None),
        out_shape=[pltpu.VMEM((1, n), jnp.float32)] * rows + [pltpu.VMEM((chips, n), jnp.float32)] * 2,
        scratch_shapes=[pltpu.VMEM((len(groups), 8, widest), jnp.float32)],
        cost_estimate=pl.CostEstimate(flops=2 * pairs * width, bytes_accessed=2 * len(blocks) * n * width, transcendentals=0),
        compiler_params=pltpu.CompilerParams(vmem_limit_bytes=VMEM_GRANT),
    )(*in_vmem([*blocks, *(state or ())]))


def merge_body(ours_ref, theirs_ref, *out_refs):
    value = jnp.maximum(ours_ref[...], theirs_ref[...])
    for k, ref in enumerate(out_refs):
        ref[...] = value[k : k + 1]


def merge(ours, theirs):
    count, n = ours.shape
    return pl.pallas_call(
        merge_body,
        out_shape=[pltpu.VMEM((1, n), jnp.float32)] * count,
        compiler_params=pltpu.CompilerParams(vmem_limit_bytes=VMEM_GRANT),
        name="merge",
    )(*in_vmem([ours, theirs]))


def solution(mesh):
    layout = Layout(mesh)
    maps = layout.line_maps()
    offsets = layout.plane_offsets()

    def send(value, pairs):
        return lax.ppermute(value, AXES, pairs)

    def nearest(embeddings, doc_order):
        n = embeddings.shape[0]
        tile = 128
        pieces = ((0, tile), (tile, n - tile))
        corner_pieces = ((0, n - tile), (n - tile, tile))
        swap = layout.swap()

        own, *parts = pack(embeddings, doc_order, pieces)
        line = []
        for hop in layout.line_hops():
            parts = [send(part, layout.line_move(hop)) for part in parts]
            line.append(parts)
        plane = [send(own, layout.plane_move(*d)) for d in offsets[:-1]]

        dy, dx = offsets[-1]
        routes = [((0, dx), (dy, 0)), ((dy, 0), (0, dx))]
        corner = []
        for k, (start, rows) in enumerate(corner_pieces):
            have, move = routes[k % 2]
            block = piece(plane[offsets.index(have)], start, rows)
            corner.append(send(block, layout.plane_move(*move)))
        twins = [send(block, swap) for block in [own, *plane]]
        corner_twins = [send(block, swap) for block in corner]

        def by_two(blocks, side):
            cols = [(block, side, k + 1, 0) for k, block in enumerate(blocks)]
            return [cols[k : k + 2] for k in range(0, len(cols), 2)]

        far = len(offsets)
        own_cols = [[(own, 0, 0, 0), (twins[0], 1, 0, 0)]]
        plane_cols, twin_cols = by_two(plane, 0), by_two(twins[1:], 1)
        corner_cols = [[(block, 0, far, start) for block, (start, _) in zip(corner, corner_pieces)]]
        ctwin_cols = [[(block, 1, far, start) for block, (start, _) in zip(corner_twins, corner_pieces)]]

        lanes = [start for start, _ in pieces]
        mine = [(own, 0, 0, False)]
        early = [(block, k + 1, at, True) for k, step in enumerate(line[:-1]) for block, at in zip(step, lanes)]
        half_a, half_b = [(block, len(line), at, True) for block, at in zip(line[-1], lanes)]
        shape = (len(line) + 1, far + 1, n)
        near_cols = own_cols + plane_cols + twin_cols
        state = match(None, [(mine, own_cols)], shape)
        if early:
            state = match(state, [(early[:1], own_cols)], shape)
        rest = [(early[1:], own_cols)] if early else []
        state = match(state, rest + [(mine + early, plane_cols)], shape)
        state = match(state, [(mine + early, twin_cols)], shape)
        state = match(state, [([half_a], near_cols)], shape)
        state = match(state, [([*mine, *early, half_a], corner_cols)], shape)
        state = match(state, [([*mine, *early, half_a], ctwin_cols)], shape)
        best = list(state[: len(line)])
        *_, late, ours, theirs = match(state, [([half_b], near_cols + corner_cols + ctwin_cols)], shape)
        best.append(late)

        theirs = send(theirs, swap)
        back = [best[0]]
        for value, m in zip(best[1:], maps):
            back.append(send(value, layout.line_return(m)))
        own_best, *others = merge(ours, theirs)
        back.append(own_best)
        for value, d in zip(others, offsets):
            back.append(send(value, backward(layout.plane_move(*d))))
        best = functools.reduce(jnp.maximum, back)
        return jnp.maximum(best, -1.0).reshape(doc_order.shape)

    return jax.shard_map(
        nearest,
        mesh=mesh,
        in_specs=(P(AXES, None), P(AXES)),
        out_specs=P(AXES),
        check_vma=False,
    )
```

```python
import functools

import jax
import jax.numpy as jnp
from jax import lax
from jax.experimental import pallas as pl
from jax.experimental.pallas import tpu as pltpu
from jax.sharding import PartitionSpec as P

AXES = ("row", "col")
CORES = 2
PAD = 8
FAR = 1.0e9
VMEM_GRANT = 16 << 20


class Layout:
    def __init__(self, mesh):
        rows, cols = mesh.shape["row"], mesh.shape["col"]
        self.xs = cols // CORES
        self.ys = self.xs if rows % self.xs == 0 else 1
        self.lines = rows // self.ys

    def index(self, line, y, x, core):
        return ((line * self.ys + y) * self.xs + x) * CORES + core

    def pairs(self, target):
        found = []
        for line in range(self.lines):
            for y in range(self.ys):
                for x in range(self.xs):
                    for core in range(CORES):
                        to = target(line, y, x, core)
                        if to is not None:
                            found.append((self.index(line, y, x, core), self.index(*to)))
        return found

    def plane_move(self, dy, dx):
        return self.pairs(lambda l, y, x, c: (l, (y + dy) % self.ys, (x + dx) % self.xs, c))

    def swap(self):
        return self.pairs(lambda l, y, x, c: (l, y, x, CORES - 1 - c))

    def plane_offsets(self):
        return [(dy, dx) for dy in range(self.ys) for dx in range(self.xs) if dy or dx]

    def line_maps(self):
        maps = []
        for step in range(1, (self.lines + 1) // 2):
            maps.append({i: (i + step) % self.lines for i in range(self.lines)})
        if self.lines % 2 == 0:
            half = self.lines // 2
            maps.append({(i if i % 2 == 0 else i + half): (i + half if i % 2 == 0 else i) for i in range(half)})
        return maps

    def line_move(self, line_map):
        return self.pairs(lambda l, y, x, c: (line_map[l], y, x, c) if l in line_map else None)

    def line_hops(self):
        return [{(b - 1) % self.lines: b for b in m.values()} for m in self.line_maps()]

    def line_return(self, line_map):
        back = {b: a for a, b in line_map.items()}
        free = [i for i in range(self.lines) if i not in line_map]
        back.update(zip([i for i in range(self.lines) if i not in back], free))
        return self.line_move(back)


def backward(pairs):
    return [(b, a) for a, b in pairs]


def pack_body(pieces, chunk, emb_hbm, order_hbm, out_ref, *refs):
    piece_refs, (emb_ref, order_ref, sems) = refs[: len(pieces)], refs[len(pieces) :]
    n, width = emb_ref.shape
    order_copy = pltpu.make_async_copy(order_hbm, order_ref, sems.at[0])
    order_copy.start()
    copies = []
    for k in range(n // chunk):
        rows = pl.ds(k * chunk, chunk)
        copies.append(pltpu.make_async_copy(emb_hbm.at[rows, :], emb_ref.at[rows, :], sems.at[k + 1]))
        copies[-1].start()
    out_ref[n:, :] = jnp.zeros((PAD, width), jnp.bfloat16)
    order_copy.wait()
    code = order_ref[...].reshape(1, n) + 1
    high = (code >> 8).astype(jnp.float32)
    low = (code & 255).astype(jnp.float32)
    line = lax.broadcasted_iota(jnp.int32, (PAD, n), 0)
    tail = jnp.where(line == 0, high, jnp.where(line == 1, low, 0.0))
    out_ref[n:, :n] = tail.astype(jnp.bfloat16)
    for k in range(n // chunk):
        copies[k].wait()
        rows = slice(k * chunk, (k + 1) * chunk)
        floats = emb_ref[rows, :].astype(jnp.float32)
        scale = lax.rsqrt(jnp.sum(floats * floats, axis=1, keepdims=True) + 1e-06)
        out_ref[rows, :] = (floats * scale).astype(jnp.bfloat16)
    for (start, rows), ref in zip(pieces, piece_refs):
        cut(out_ref, start, rows, ref)


def pack(embeddings, doc_order, pieces):
    n, width = embeddings.shape
    chunk = 128 if n % 128 == 0 else n
    call = pl.pallas_call(
        functools.partial(pack_body, pieces, chunk),
        in_specs=[pl.BlockSpec(memory_space=pltpu.HBM)] * 2,
        out_shape=[pltpu.VMEM((rows + PAD, width), jnp.bfloat16) for rows in (n, *(rows for _, rows in pieces))],
        scratch_shapes=[
            pltpu.VMEM((n, width), jnp.bfloat16),
            pltpu.VMEM((n,), jnp.int32),
            pltpu.SemaphoreType.DMA((n // chunk + 1,)),
        ],
        compiler_params=pltpu.CompilerParams(vmem_limit_bytes=VMEM_GRANT),
        name="pack",
    )
    return call(*(pltpu.with_memory_space_constraint(v, pltpu.HBM) for v in (embeddings, doc_order)))


def cut(ref, start, rows, out_ref):
    n = ref.shape[0] - PAD
    out_ref[:rows, :] = ref[start : start + rows, :]
    out_ref[rows:, :] = jnp.zeros((PAD, ref.shape[1]), jnp.bfloat16)
    out_ref[rows:, :rows] = ref[n:, start : start + rows]


def piece_body(start, rows, ref, out_ref):
    cut(ref, start, rows, out_ref)


def piece(block, start, rows):
    return pl.pallas_call(
        functools.partial(piece_body, start, rows),
        out_shape=pltpu.VMEM((rows + PAD, block.shape[1]), jnp.bfloat16),
        compiler_params=pltpu.CompilerParams(vmem_limit_bytes=VMEM_GRANT),
        name="piece",
    )(*in_vmem([block]))


def lane_orders(ref):
    n = ref.shape[0] - PAD
    tail = ref[n:, :n].astype(jnp.float32)
    order = tail[0:1] * 256.0 + tail[1:2]
    return jnp.where(order == 0.0, FAR, order)


def match_body(tasks, groups, n_blocks, initial, *refs):
    blocks, refs = refs[:n_blocks], refs[n_blocks:]
    count = len(refs) - 1 if initial else len(refs) // 2
    before, after, col_acc = refs[: len(refs) - count - 1], refs[-count - 1 : -1], refs[-1]
    lanes = 128
    for k, ref in enumerate(after):
        ref[...] = jnp.full(ref.shape, -1.0, jnp.float32) if initial else before[k][...]

    def units_of(numbers):
        parts = [blocks[k][: blocks[k].shape[0] - PAD, :] for k in numbers]
        return parts[0] if len(parts) == 1 else jnp.concatenate(parts, axis=0)

    def settle(value, block, place):
        orders = lane_orders(blocks[block])
        result, row, lane = place
        at = (slice(row, row + 1), slice(lane, lane + orders.shape[1]))
        after[result][at] = jnp.maximum(after[result][at], jnp.where(orders == FAR, -1.0, value))

    fresh = set()
    for rows, meets in tasks:
        row_units = units_of([row[0] for row in rows])
        sizes = [blocks[row[0]].shape[0] - PAD for row in rows]
        columns = [jnp.broadcast_to(lane_orders(blocks[row[0]]), (lanes, n)).T[:, 0:1] for row, n in zip(rows, sizes)]
        best = [jnp.full((n, lanes), -1.0, jnp.float32) for n in sizes]
        gives = any(row[2] for row in rows)
        for g in meets:
            numbers = [col[0] for col in groups[g]]
            orders = jnp.concatenate([lane_orders(blocks[k]) for k in numbers], axis=1)
            score = lax.dot_general(
                row_units, units_of(numbers), (((1,), (1,)), ((), ())), preferred_element_type=jnp.float32
            )
            for k in range(0, score.shape[1], lanes):
                first = 0
                kept = [col_acc[g, :, k : k + lanes]] if g in fresh else []
                for r, n in enumerate(sizes):
                    part = score[first : first + n, k : k + lanes]
                    earlier = orders[:, k : k + lanes] < columns[r]
                    best[r] = jnp.maximum(best[r], jnp.where(earlier, part, -1.0))
                    if rows[r][2]:
                        kept.append(jnp.max(jnp.where(earlier, -1.0, part).reshape(n // 8, 8, lanes), axis=0))
                    first += n
                if gives:
                    col_acc[g, :, k : k + lanes] = functools.reduce(jnp.maximum, kept)
            if gives:
                fresh.add(g)
        for r, (block, place, _) in enumerate(rows):
            settle(jnp.max(best[r].T, axis=0, keepdims=True), block, place)
    for g in sorted(fresh):
        start = 0
        for block, place in groups[g]:
            n = blocks[block].shape[0] - PAD
            settle(jnp.max(col_acc[g, :, start : start + n], axis=0, keepdims=True), block, place)
            start += n


def in_vmem(values):
    return [pltpu.with_memory_space_constraint(v, pltpu.VMEM) for v in values]


def match(state, tasks, shape):
    blocks, groups, plan = [], [], []

    def number(value):
        for k, known in enumerate(blocks):
            if known is value:
                return k
        blocks.append(value)
        return len(blocks) - 1

    for rows, meets in tasks:
        found = []
        for group in meets:
            group = [(number(block), place) for block, place in group]
            if group not in groups:
                groups.append(group)
            found.append(groups.index(group))
        plan.append(([(number(row), *rest) for row, *rest in rows], found))
    rows, chips, n = shape
    width = blocks[0].shape[1]
    widest = max(sum(blocks[col[0]].shape[0] - PAD for col in group) for group in groups)
    pairs = sum(blocks[r[0]].shape[0] * blocks[col[0]].shape[0] for p in plan for r in p[0] for g in p[1] for col in groups[g])
    return pl.pallas_call(
        functools.partial(match_body, plan, groups, len(blocks), state is None),
        out_shape=[pltpu.VMEM((1, n), jnp.float32)] * rows + [pltpu.VMEM((chips, n), jnp.float32)] * 2,
        scratch_shapes=[pltpu.VMEM((len(groups), 8, widest), jnp.float32)],
        cost_estimate=pl.CostEstimate(flops=2 * pairs * width, bytes_accessed=2 * len(blocks) * n * width, transcendentals=0),
        compiler_params=pltpu.CompilerParams(vmem_limit_bytes=VMEM_GRANT),
    )(*in_vmem([*blocks, *(state or ())]))


def merge_body(ours_ref, theirs_ref, *out_refs):
    value = jnp.maximum(ours_ref[...], theirs_ref[...])
    for k, ref in enumerate(out_refs):
        ref[...] = value[k : k + 1]


def merge(ours, theirs):
    count, n = ours.shape
    return pl.pallas_call(
        merge_body,
        out_shape=[pltpu.VMEM((1, n), jnp.float32)] * count,
        compiler_params=pltpu.CompilerParams(vmem_limit_bytes=VMEM_GRANT),
        name="merge",
    )(*in_vmem([ours, theirs]))


def solution(mesh):
    layout = Layout(mesh)
    maps = layout.line_maps()
    offsets = layout.plane_offsets()

    def send(value, pairs):
        return lax.ppermute(value, AXES, pairs)

    def nearest(embeddings, doc_order):
        n = embeddings.shape[0]
        tile = 128
        pieces = ((0, tile), (tile, n - tile))
        corner_pieces = ((0, n - tile), (n - tile, tile))
        swap = layout.swap()

        own, *parts = pack(embeddings, doc_order, pieces)
        line = []
        for hop in layout.line_hops():
            parts = [send(part, layout.line_move(hop)) for part in parts]
            line.append(parts)
        plane = [send(own, layout.plane_move(*d)) for d in offsets[:-1]]

        dy, dx = offsets[-1]
        routes = [((0, dx), (dy, 0)), ((dy, 0), (0, dx))]
        corner = []
        for k, (start, rows) in enumerate(corner_pieces):
            have, move = routes[k % 2]
            block = piece(plane[offsets.index(have)], start, rows)
            corner.append(send(block, layout.plane_move(*move)))
        twins = [send(block, swap) for block in [own, *plane]]
        corner_twins = [send(block, swap) for block in corner]

        far = len(offsets)
        shape = (len(line) + 1, far + 1, n)
        side_of = [len(line) + 1, len(line) + 2]

        def by_two(blocks, side):
            cols = [(block, (side_of[side], k + 1, 0)) for k, block in enumerate(blocks)]
            return [cols[k : k + 2] for k in range(0, len(cols), 2)]

        own_cols = [[(own, (side_of[0], 0, 0)), (twins[0], (side_of[1], 0, 0))]]
        plane_cols, twin_cols = by_two(plane, 0), by_two(twins[1:], 1)
        corner_cols, ctwin_cols = (
            [[(block, (side_of[side], far, start)) for block, (start, _) in zip(blocks, corner_pieces)]]
            for side, blocks in enumerate((corner, corner_twins))
        )
        lanes = [start for start, _ in pieces]
        mine = [(own, (0, 0, 0), False)]
        early = [(block, (k + 1, 0, at), True) for k, step in enumerate(line[:-1]) for block, at in zip(step, lanes)]
        half_a, half_b = [(block, (len(line), 0, at), True) for block, at in zip(line[-1], lanes)]

        def streamed(groups):
            return [(*col, True) for group in groups for col in group]

        near = streamed(own_cols + plane_cols + twin_cols)
        state = match(None, [(mine, own_cols)], shape)
        if early:
            state = match(state, [(early[:1], own_cols)], shape)
        rest = [(early[1:], own_cols)] if early else []
        state = match(state, rest + [(mine + early, plane_cols)], shape)
        state = match(state, [(mine + early, twin_cols)], shape)
        state = match(state, [(near, [[half_a[:2]]])], shape)
        state = match(state, [([*mine, *early, half_a], corner_cols)], shape)
        state = match(state, [([*mine, *early, half_a], ctwin_cols)], shape)
        best = list(state[: len(line)])
        everything = near + streamed(corner_cols + ctwin_cols)
        *_, late, ours, theirs = match(state, [(everything, [[half_b[:2]]])], shape)
        best.append(late)

        theirs = send(theirs, swap)
        back = [best[0]]
        for value, m in zip(best[1:], maps):
            back.append(send(value, layout.line_return(m)))
        own_best, *others = merge(ours, theirs)
        back.append(own_best)
        for value, d in zip(others, offsets):
            back.append(send(value, backward(layout.plane_move(*d))))
        best = functools.reduce(jnp.maximum, back)
        return jnp.maximum(best, -1.0).reshape(doc_order.shape)

    return jax.shard_map(
        nearest,
        mesh=mesh,
        in_specs=(P(AXES, None), P(AXES)),
        out_specs=P(AXES),
        check_vma=False,
    )
```

```python
import functools

import jax
import jax.numpy as jnp
from jax import lax
from jax.experimental import pallas as pl
from jax.experimental.pallas import tpu as pltpu
from jax.sharding import PartitionSpec as P

AXES = ("row", "col")
CORES = 2
PAD = 8
FAR = 1.0e9
VMEM_GRANT = 16 << 20


class Layout:
    def __init__(self, mesh):
        rows, cols = mesh.shape["row"], mesh.shape["col"]
        self.xs = cols // CORES
        self.ys = self.xs if rows % self.xs == 0 else 1
        self.lines = rows // self.ys

    def index(self, line, y, x, core):
        return ((line * self.ys + y) * self.xs + x) * CORES + core

    def pairs(self, target):
        found = []
        for line in range(self.lines):
            for y in range(self.ys):
                for x in range(self.xs):
                    for core in range(CORES):
                        to = target(line, y, x, core)
                        if to is not None:
                            found.append((self.index(line, y, x, core), self.index(*to)))
        return found

    def plane_move(self, dy, dx):
        return self.pairs(lambda l, y, x, c: (l, (y + dy) % self.ys, (x + dx) % self.xs, c))

    def swap(self):
        return self.pairs(lambda l, y, x, c: (l, y, x, CORES - 1 - c))

    def plane_offsets(self):
        return [(dy, dx) for dy in range(self.ys) for dx in range(self.xs) if dy or dx]

    def line_maps(self):
        maps = []
        for step in range(1, (self.lines + 1) // 2):
            maps.append({i: (i + step) % self.lines for i in range(self.lines)})
        if self.lines % 2 == 0:
            half = self.lines // 2
            maps.append({(i if i % 2 == 0 else i + half): (i + half if i % 2 == 0 else i) for i in range(half)})
        return maps

    def line_move(self, line_map):
        return self.pairs(lambda l, y, x, c: (line_map[l], y, x, c) if l in line_map else None)

    def line_hops(self):
        return [{(b - 1) % self.lines: b for b in m.values()} for m in self.line_maps()]

    def line_return(self, line_map):
        back = {b: a for a, b in line_map.items()}
        free = [i for i in range(self.lines) if i not in line_map]
        back.update(zip([i for i in range(self.lines) if i not in back], free))
        return self.line_move(back)


def backward(pairs):
    return [(b, a) for a, b in pairs]


def pack_body(pieces, chunk, emb_hbm, order_hbm, out_ref, *refs):
    piece_refs, (emb_ref, order_ref, sems) = refs[: len(pieces)], refs[len(pieces) :]
    n, width = emb_ref.shape
    order_copy = pltpu.make_async_copy(order_hbm, order_ref, sems.at[0])
    order_copy.start()
    copies = []
    for k in range(n // chunk):
        rows = pl.ds(k * chunk, chunk)
        copies.append(pltpu.make_async_copy(emb_hbm.at[rows, :], emb_ref.at[rows, :], sems.at[k + 1]))
        copies[-1].start()
    out_ref[n:, :] = jnp.zeros((PAD, width), jnp.bfloat16)
    order_copy.wait()
    code = order_ref[...].reshape(1, n) + 1
    high = (code >> 8).astype(jnp.float32)
    low = (code & 255).astype(jnp.float32)
    line = lax.broadcasted_iota(jnp.int32, (PAD, n), 0)
    tail = jnp.where(line == 0, high, jnp.where(line == 1, low, 0.0))
    out_ref[n:, :n] = tail.astype(jnp.bfloat16)
    for k in range(n // chunk):
        copies[k].wait()
        rows = slice(k * chunk, (k + 1) * chunk)
        floats = emb_ref[rows, :].astype(jnp.float32)
        scale = lax.rsqrt(jnp.sum(floats * floats, axis=1, keepdims=True) + 1e-06)
        out_ref[rows, :] = (floats * scale).astype(jnp.bfloat16)
    for (start, rows), ref in zip(pieces, piece_refs):
        cut(out_ref, start, rows, ref)


def pack(embeddings, doc_order, pieces):
    n, width = embeddings.shape
    chunk = 128 if n % 128 == 0 else n
    call = pl.pallas_call(
        functools.partial(pack_body, pieces, chunk),
        in_specs=[pl.BlockSpec(memory_space=pltpu.HBM)] * 2,
        out_shape=[pltpu.VMEM((rows + PAD, width), jnp.bfloat16) for rows in (n, *(rows for _, rows in pieces))],
        scratch_shapes=[
            pltpu.VMEM((n, width), jnp.bfloat16),
            pltpu.VMEM((n,), jnp.int32),
            pltpu.SemaphoreType.DMA((n // chunk + 1,)),
        ],
        compiler_params=pltpu.CompilerParams(vmem_limit_bytes=VMEM_GRANT),
        name="pack",
    )
    return call(*(pltpu.with_memory_space_constraint(v, pltpu.HBM) for v in (embeddings, doc_order)))


def cut(ref, start, rows, out_ref):
    n = ref.shape[0] - PAD
    out_ref[:rows, :] = ref[start : start + rows, :]
    out_ref[rows:, :] = jnp.zeros((PAD, ref.shape[1]), jnp.bfloat16)
    out_ref[rows:, :rows] = ref[n:, start : start + rows]


def piece_body(start, rows, ref, out_ref):
    cut(ref, start, rows, out_ref)


def piece(block, start, rows):
    return pl.pallas_call(
        functools.partial(piece_body, start, rows),
        out_shape=pltpu.VMEM((rows + PAD, block.shape[1]), jnp.bfloat16),
        compiler_params=pltpu.CompilerParams(vmem_limit_bytes=VMEM_GRANT),
        name="piece",
    )(*in_vmem([block]))


def lane_orders(ref):
    n = ref.shape[0] - PAD
    tail = ref[n:, :n].astype(jnp.float32)
    order = tail[0:1] * 256.0 + tail[1:2]
    return jnp.where(order == 0.0, FAR, order)


def match_body(tasks, groups, n_blocks, initial, needed, *refs):
    blocks, refs = refs[:n_blocks], refs[n_blocks:]
    count = len(refs) - 1 if initial else len(refs) // 2
    before, after, col_acc = refs[: len(refs) - count - 1], refs[-count - 1 : -1], refs[-1]
    lanes = 128
    for k, ref in enumerate(after):
        ref[...] = jnp.full(ref.shape, -1.0, jnp.float32) if initial else before[k][...]

    def work():
        def units_of(numbers):
            parts = [blocks[k][: blocks[k].shape[0] - PAD, :] for k in numbers]
            return parts[0] if len(parts) == 1 else jnp.concatenate(parts, axis=0)

        def settle(value, block, place):
            orders = lane_orders(blocks[block])
            result, row, lane = place
            at = (slice(row, row + 1), slice(lane, lane + orders.shape[1]))
            after[result][at] = jnp.maximum(after[result][at], jnp.where(orders == FAR, -1.0, value))

        fresh = set()
        for rows, meets in tasks:
            row_units = units_of([row[0] for row in rows])
            sizes = [blocks[row[0]].shape[0] - PAD for row in rows]
            columns = [jnp.broadcast_to(lane_orders(blocks[row[0]]), (lanes, n)).T[:, 0:1] for row, n in zip(rows, sizes)]
            best = [jnp.full((n, lanes), -1.0, jnp.float32) for n in sizes]
            gives = any(row[2] for row in rows)
            for g in meets:
                numbers = [col[0] for col in groups[g]]
                orders = jnp.concatenate([lane_orders(blocks[k]) for k in numbers], axis=1)
                score = lax.dot_general(
                    row_units, units_of(numbers), (((1,), (1,)), ((), ())), preferred_element_type=jnp.float32
                )
                for k in range(0, score.shape[1], lanes):
                    first = 0
                    kept = [col_acc[g, :, k : k + lanes]] if g in fresh else []
                    for r, n in enumerate(sizes):
                        part = score[first : first + n, k : k + lanes]
                        earlier = orders[:, k : k + lanes] < columns[r]
                        best[r] = jnp.maximum(best[r], jnp.where(earlier, part, -1.0))
                        if rows[r][2]:
                            kept.append(jnp.max(jnp.where(earlier, -1.0, part).reshape(n // 8, 8, lanes), axis=0))
                        first += n
                    if gives:
                        col_acc[g, :, k : k + lanes] = functools.reduce(jnp.maximum, kept)
                if gives:
                    fresh.add(g)
            for r, (block, place, _) in enumerate(rows):
                settle(jnp.max(best[r].T, axis=0, keepdims=True), block, place)
        for g in sorted(fresh):
            start = 0
            for block, place in groups[g]:
                n = blocks[block].shape[0] - PAD
                settle(jnp.max(col_acc[g, :, start : start + n], axis=0, keepdims=True), block, place)
                start += n

    if needed is None:
        work()
    else:
        pl.when(jnp.min(lane_orders(blocks[needed])) < FAR)(work)


def in_vmem(values):
    return [pltpu.with_memory_space_constraint(v, pltpu.VMEM) for v in values]


def match(state, tasks, shape, needed=None):
    blocks, groups, plan = [], [], []

    def number(value):
        for k, known in enumerate(blocks):
            if known is value:
                return k
        blocks.append(value)
        return len(blocks) - 1

    for rows, meets in tasks:
        found = []
        for group in meets:
            group = [(number(block), place) for block, place in group]
            if group not in groups:
                groups.append(group)
            found.append(groups.index(group))
        plan.append(([(number(row), *rest) for row, *rest in rows], found))
    rows, chips, n = shape
    width = blocks[0].shape[1]
    widest = max(sum(blocks[col[0]].shape[0] - PAD for col in group) for group in groups)
    pairs = sum(blocks[r[0]].shape[0] * blocks[col[0]].shape[0] for p in plan for r in p[0] for g in p[1] for col in groups[g])
    return pl.pallas_call(
        functools.partial(match_body, plan, groups, len(blocks), state is None, None if needed is None else number(needed)),
        out_shape=[pltpu.VMEM((1, n), jnp.float32)] * rows + [pltpu.VMEM((chips, n), jnp.float32)] * 2,
        scratch_shapes=[pltpu.VMEM((len(groups), 8, widest), jnp.float32)],
        cost_estimate=pl.CostEstimate(flops=2 * pairs * width, bytes_accessed=2 * len(blocks) * n * width, transcendentals=0),
        compiler_params=pltpu.CompilerParams(vmem_limit_bytes=VMEM_GRANT),
    )(*in_vmem([*blocks, *(state or ())]))


def merge_body(ours_ref, theirs_ref, *out_refs):
    value = jnp.maximum(ours_ref[...], theirs_ref[...])
    for k, ref in enumerate(out_refs):
        ref[...] = value[k : k + 1]


def merge(ours, theirs):
    count, n = ours.shape
    return pl.pallas_call(
        merge_body,
        out_shape=[pltpu.VMEM((1, n), jnp.float32)] * count,
        compiler_params=pltpu.CompilerParams(vmem_limit_bytes=VMEM_GRANT),
        name="merge",
    )(*in_vmem([ours, theirs]))


def solution(mesh):
    layout = Layout(mesh)
    maps = layout.line_maps()
    offsets = layout.plane_offsets()

    def send(value, pairs):
        return lax.ppermute(value, AXES, pairs)

    def nearest(embeddings, doc_order):
        n = embeddings.shape[0]
        tile = 128
        pieces = ((0, tile), (tile, n - tile))
        corner_pieces = ((0, n - tile), (n - tile, tile))
        swap = layout.swap()

        own, *parts = pack(embeddings, doc_order, pieces)
        line = []
        for hop in layout.line_hops()[:-1]:
            source = line[-1] if line else parts
            line.append([send(part, layout.line_move(hop)) for part in source])
        line.append([send(part, layout.line_move(maps[-1])) for part in parts])
        plane = [send(own, layout.plane_move(*d)) for d in offsets[:-1]]

        dy, dx = offsets[-1]
        routes = [((0, dx), (dy, 0)), ((dy, 0), (0, dx))]
        corner = []
        for k, (start, rows) in enumerate(corner_pieces):
            have, move = routes[k % 2]
            block = piece(plane[offsets.index(have)], start, rows)
            corner.append(send(block, layout.plane_move(*move)))
        twins = [send(block, swap) for block in [own, *plane]]
        corner_twins = [send(block, swap) for block in corner]

        far = len(offsets)
        shape = (len(line) + 1, far + 1, n)
        side_of = [len(line) + 1, len(line) + 2]

        def by_two(blocks, side):
            cols = [(block, (side_of[side], k + 1, 0)) for k, block in enumerate(blocks)]
            return [cols[k : k + 2] for k in range(0, len(cols), 2)]

        own_cols = [[(own, (side_of[0], 0, 0)), (twins[0], (side_of[1], 0, 0))]]
        plane_cols, twin_cols = by_two(plane, 0), by_two(twins[1:], 1)
        corner_cols, ctwin_cols = (
            [[(block, (side_of[side], far, start)) for block, (start, _) in zip(blocks, corner_pieces)]]
            for side, blocks in enumerate((corner, corner_twins))
        )
        lanes = [start for start, _ in pieces]
        mine = [(own, (0, 0, 0), False)]
        early = [(block, (k + 1, 0, at), True) for k, step in enumerate(line[:-1]) for block, at in zip(step, lanes)]
        half_a, half_b = [(block, (len(line), 0, at), True) for block, at in zip(line[-1], lanes)]

        def streamed(groups):
            return [(*col, True) for group in groups for col in group]

        near = streamed(own_cols + plane_cols + twin_cols)
        state = match(None, [(mine, own_cols)], shape)
        if early:
            state = match(state, [(early[:1], own_cols)], shape)
        rest = [(early[1:], own_cols)] if early else []
        state = match(state, rest + [(mine + early, plane_cols)], shape)
        state = match(state, [(mine + early, twin_cols)], shape)
        state = match(state, [(near, [[half_a[:2]]])], shape, half_a[0])
        state = match(state, [([*mine, *early, half_a], corner_cols)], shape)
        state = match(state, [([*mine, *early, half_a], ctwin_cols)], shape)
        best = list(state[: len(line)])
        shift = len(line)
        streams = [(b, (at[0] - shift, *at[1:]), gives) for b, at, gives in near + streamed(corner_cols + ctwin_cols)]
        piece_at = (half_b[0], (0, *half_b[1][1:]))
        late, ours, theirs = match(state[shift:], [(streams, [[piece_at]])], (1, *shape[1:]), half_b[0])
        best.append(late)

        theirs = send(theirs, swap)
        back = [best[0]]
        for value, m in zip(best[1:], maps):
            back.append(send(value, layout.line_return(m)))
        own_best, *others = merge(ours, theirs)
        back.append(own_best)
        for value, d in zip(others, offsets):
            back.append(send(value, backward(layout.plane_move(*d))))
        best = functools.reduce(jnp.maximum, back)
        return jnp.maximum(best, -1.0).reshape(doc_order.shape)

    return jax.shard_map(
        nearest,
        mesh=mesh,
        in_specs=(P(AXES, None), P(AXES)),
        out_specs=P(AXES),
        check_vma=False,
    )
```

```python
import functools

import jax
import jax.numpy as jnp
from jax import lax
from jax.experimental import pallas as pl
from jax.experimental.pallas import tpu as pltpu
from jax.sharding import PartitionSpec as P

AXES = ("row", "col")
CORES = 2
PAD = 8
FAR = 1.0e9
VMEM_GRANT = 16 << 20


class Layout:
    def __init__(self, mesh):
        rows, cols = mesh.shape["row"], mesh.shape["col"]
        self.xs = cols // CORES
        self.ys = self.xs if rows % self.xs == 0 else 1
        self.lines = rows // self.ys

    def index(self, line, y, x, core):
        return ((line * self.ys + y) * self.xs + x) * CORES + core

    def pairs(self, target):
        found = []
        for line in range(self.lines):
            for y in range(self.ys):
                for x in range(self.xs):
                    for core in range(CORES):
                        to = target(line, y, x, core)
                        if to is not None:
                            found.append((self.index(line, y, x, core), self.index(*to)))
        return found

    def plane_move(self, dy, dx):
        return self.pairs(lambda l, y, x, c: (l, (y + dy) % self.ys, (x + dx) % self.xs, c))

    def swap(self):
        return self.pairs(lambda l, y, x, c: (l, y, x, CORES - 1 - c))

    def plane_offsets(self):
        return [(dy, dx) for dy in range(self.ys) for dx in range(self.xs) if dy or dx]

    def line_maps(self):
        maps = []
        for step in range(1, (self.lines + 1) // 2):
            maps.append({i: (i + step) % self.lines for i in range(self.lines)})
        if self.lines % 2 == 0:
            half = self.lines // 2
            maps.append({(i if i % 2 == 0 else i + half): (i + half if i % 2 == 0 else i) for i in range(half)})
        return maps

    def line_move(self, line_map):
        return self.pairs(lambda l, y, x, c: (line_map[l], y, x, c) if l in line_map else None)

    def line_hops(self):
        return [{(b - 1) % self.lines: b for b in m.values()} for m in self.line_maps()]

    def line_return(self, line_map):
        back = {b: a for a, b in line_map.items()}
        free = [i for i in range(self.lines) if i not in line_map]
        back.update(zip([i for i in range(self.lines) if i not in back], free))
        return self.line_move(back)


def backward(pairs):
    return [(b, a) for a, b in pairs]


def pack_body(pieces, chunk, emb_hbm, order_hbm, out_ref, *refs):
    piece_refs, (emb_ref, order_ref, sems) = refs[: len(pieces)], refs[len(pieces) :]
    n, width = emb_ref.shape
    order_copy = pltpu.make_async_copy(order_hbm, order_ref, sems.at[0])
    order_copy.start()
    copies = []
    for k in range(n // chunk):
        rows = pl.ds(k * chunk, chunk)
        copies.append(pltpu.make_async_copy(emb_hbm.at[rows, :], emb_ref.at[rows, :], sems.at[k + 1]))
        copies[-1].start()
    out_ref[n:, :] = jnp.zeros((PAD, width), jnp.bfloat16)
    order_copy.wait()
    code = order_ref[...].reshape(1, n) + 1
    high = (code >> 8).astype(jnp.float32)
    low = (code & 255).astype(jnp.float32)
    line = lax.broadcasted_iota(jnp.int32, (PAD, n), 0)
    tail = jnp.where(line == 0, high, jnp.where(line == 1, low, 0.0))
    out_ref[n:, :n] = tail.astype(jnp.bfloat16)
    for k in range(n // chunk):
        copies[k].wait()
        rows = slice(k * chunk, (k + 1) * chunk)
        floats = emb_ref[rows, :].astype(jnp.float32)
        scale = lax.rsqrt(jnp.sum(floats * floats, axis=1, keepdims=True) + 1e-06)
        out_ref[rows, :] = (floats * scale).astype(jnp.bfloat16)
    for (start, rows), ref in zip(pieces, piece_refs):
        cut(out_ref, start, rows, ref)


def pack(embeddings, doc_order, pieces):
    n, width = embeddings.shape
    chunk = 128 if n % 128 == 0 else n
    call = pl.pallas_call(
        functools.partial(pack_body, pieces, chunk),
        in_specs=[pl.BlockSpec(memory_space=pltpu.HBM)] * 2,
        out_shape=[pltpu.VMEM((rows + PAD, width), jnp.bfloat16) for rows in (n, *(rows for _, rows in pieces))],
        scratch_shapes=[
            pltpu.VMEM((n, width), jnp.bfloat16),
            pltpu.VMEM((n,), jnp.int32),
            pltpu.SemaphoreType.DMA((n // chunk + 1,)),
        ],
        compiler_params=pltpu.CompilerParams(vmem_limit_bytes=VMEM_GRANT),
        name="pack",
    )
    return call(*(pltpu.with_memory_space_constraint(v, pltpu.HBM) for v in (embeddings, doc_order)))


def cut(ref, start, rows, out_ref):
    n = ref.shape[0] - PAD
    out_ref[:rows, :] = ref[start : start + rows, :]
    out_ref[rows:, :] = jnp.zeros((PAD, ref.shape[1]), jnp.bfloat16)
    out_ref[rows:, :rows] = ref[n:, start : start + rows]


def piece_body(start, rows, ref, out_ref):
    cut(ref, start, rows, out_ref)


def piece(block, start, rows):
    return pl.pallas_call(
        functools.partial(piece_body, start, rows),
        out_shape=pltpu.VMEM((rows + PAD, block.shape[1]), jnp.bfloat16),
        compiler_params=pltpu.CompilerParams(vmem_limit_bytes=VMEM_GRANT),
        name="piece",
    )(*in_vmem([block]))


def lane_orders(ref):
    n = ref.shape[0] - PAD
    tail = ref[n:, :n].astype(jnp.float32)
    order = tail[0:1] * 256.0 + tail[1:2]
    return jnp.where(order == 0.0, FAR, order)


def match_body(tasks, groups, n_blocks, initial, needed, *refs):
    blocks, refs = refs[:n_blocks], refs[n_blocks:]
    count = len(refs) - 1 if initial else len(refs) // 2
    before, after, col_acc = refs[: len(refs) - count - 1], refs[-count - 1 : -1], refs[-1]
    lanes = 128
    for k, ref in enumerate(after):
        ref[...] = jnp.full(ref.shape, -1.0, jnp.float32) if initial else before[k][...]

    def work():
        def units_of(numbers):
            parts = [blocks[k][: blocks[k].shape[0] - PAD, :] for k in numbers]
            return parts[0] if len(parts) == 1 else jnp.concatenate(parts, axis=0)

        def settle(value, block, place):
            orders = lane_orders(blocks[block])
            result, row, lane = place
            at = (slice(row, row + 1), slice(lane, lane + orders.shape[1]))
            after[result][at] = jnp.maximum(after[result][at], jnp.where(orders == FAR, -1.0, value))

        fresh = set()
        for rows, meets in tasks:
            row_units = units_of([row[0] for row in rows])
            sizes = [blocks[row[0]].shape[0] - PAD for row in rows]
            columns = [jnp.broadcast_to(lane_orders(blocks[row[0]]), (lanes, n)).T[:, 0:1] for row, n in zip(rows, sizes)]
            best = [jnp.full((n, lanes), -1.0, jnp.float32) for n in sizes]
            gives = any(row[2] for row in rows)
            for g in meets:
                numbers = [col[0] for col in groups[g]]
                orders = jnp.concatenate([lane_orders(blocks[k]) for k in numbers], axis=1)
                score = lax.dot_general(
                    row_units, units_of(numbers), (((1,), (1,)), ((), ())), preferred_element_type=jnp.float32
                )
                for k in range(0, score.shape[1], lanes):
                    first = 0
                    kept = [col_acc[g, :, k : k + lanes]] if g in fresh else []
                    for r, n in enumerate(sizes):
                        part = score[first : first + n, k : k + lanes]
                        earlier = orders[:, k : k + lanes] < columns[r]
                        best[r] = jnp.maximum(best[r], jnp.where(earlier, part, -1.0))
                        if rows[r][2]:
                            kept.append(jnp.max(jnp.where(earlier, -1.0, part).reshape(n // 8, 8, lanes), axis=0))
                        first += n
                    if gives:
                        col_acc[g, :, k : k + lanes] = functools.reduce(jnp.maximum, kept)
                if gives:
                    fresh.add(g)
            for r, (block, place, _) in enumerate(rows):
                settle(jnp.max(best[r].T, axis=0, keepdims=True), block, place)
        for g in sorted(fresh):
            start = 0
            for block, place in groups[g]:
                n = blocks[block].shape[0] - PAD
                settle(jnp.max(col_acc[g, :, start : start + n], axis=0, keepdims=True), block, place)
                start += n

    if needed is None:
        work()
    else:
        pl.when(jnp.min(lane_orders(blocks[needed])) < FAR)(work)


def in_vmem(values):
    return [pltpu.with_memory_space_constraint(v, pltpu.VMEM) for v in values]


def match(state, tasks, shape, needed=None):
    blocks, groups, plan = [], [], []

    def number(value):
        for k, known in enumerate(blocks):
            if known is value:
                return k
        blocks.append(value)
        return len(blocks) - 1

    for rows, meets in tasks:
        found = []
        for group in meets:
            group = [(number(block), place) for block, place in group]
            if group not in groups:
                groups.append(group)
            found.append(groups.index(group))
        plan.append(([(number(row), *rest) for row, *rest in rows], found))
    rows, chips, n = shape
    width = blocks[0].shape[1]
    widest = max(sum(blocks[col[0]].shape[0] - PAD for col in group) for group in groups)
    pairs = sum(blocks[r[0]].shape[0] * blocks[col[0]].shape[0] for p in plan for r in p[0] for g in p[1] for col in groups[g])
    return pl.pallas_call(
        functools.partial(match_body, plan, groups, len(blocks), state is None, None if needed is None else number(needed)),
        out_shape=[pltpu.VMEM((1, n), jnp.float32)] * rows + [pltpu.VMEM((chips, n), jnp.float32)] * 2,
        scratch_shapes=[pltpu.VMEM((len(groups), 8, widest), jnp.float32)],
        cost_estimate=pl.CostEstimate(flops=2 * pairs * width, bytes_accessed=2 * len(blocks) * n * width, transcendentals=0),
        compiler_params=pltpu.CompilerParams(vmem_limit_bytes=VMEM_GRANT),
    )(*in_vmem([*blocks, *(state or ())]))


def merge_body(ours_ref, theirs_ref, *out_refs):
    value = jnp.maximum(ours_ref[...], theirs_ref[...])
    for k, ref in enumerate(out_refs):
        ref[...] = value[k : k + 1]


def merge(ours, theirs):
    count, n = ours.shape
    return pl.pallas_call(
        merge_body,
        out_shape=[pltpu.VMEM((1, n), jnp.float32)] * count,
        compiler_params=pltpu.CompilerParams(vmem_limit_bytes=VMEM_GRANT),
        name="merge",
    )(*in_vmem([ours, theirs]))


def solution(mesh):
    layout = Layout(mesh)
    maps = layout.line_maps()
    offsets = layout.plane_offsets()

    def send(value, pairs):
        return lax.ppermute(value, AXES, pairs)

    def nearest(embeddings, doc_order):
        n = embeddings.shape[0]
        tile = 128
        pieces = ((0, tile), (tile, n - tile))
        corner_pieces = ((0, n - tile), (n - tile, tile))
        swap = layout.swap()

        own, *parts = pack(embeddings, doc_order, pieces)
        line = [[own]]
        for hop in layout.line_hops()[:-1]:
            line.append([send(line[-1][0], layout.line_move(hop))])
        line = line[1:]
        line.append([send(part, layout.line_move(maps[-1])) for part in parts])
        plane = [send(own, layout.plane_move(*d)) for d in offsets[:-1]]

        dy, dx = offsets[-1]
        routes = [((0, dx), (dy, 0)), ((dy, 0), (0, dx))]
        corner = []
        for k, (start, rows) in enumerate(corner_pieces):
            have, move = routes[k % 2]
            block = piece(plane[offsets.index(have)], start, rows)
            corner.append(send(block, layout.plane_move(*move)))
        twins = [send(block, swap) for block in [own, *plane]]
        corner_twins = [send(block, swap) for block in corner]

        far = len(offsets)
        shape = (len(line) + 1, far + 1, n)
        side_of = [len(line) + 1, len(line) + 2]

        def by_two(blocks, side):
            cols = [(block, (side_of[side], k + 1, 0)) for k, block in enumerate(blocks)]
            return [cols[k : k + 2] for k in range(0, len(cols), 2)]

        own_cols = [[(own, (side_of[0], 0, 0)), (twins[0], (side_of[1], 0, 0))]]
        plane_cols, twin_cols = by_two(plane, 0), by_two(twins[1:], 1)
        corner_cols, ctwin_cols = (
            [[(block, (side_of[side], far, start)) for block, (start, _) in zip(blocks, corner_pieces)]]
            for side, blocks in enumerate((corner, corner_twins))
        )
        lanes = [start for start, _ in pieces]
        mine = [(own, (0, 0, 0), False)]
        early = [(step[0], (k + 1, 0, 0), True) for k, step in enumerate(line[:-1])]
        half_a, half_b = [(block, (len(line), 0, at), True) for block, at in zip(line[-1], lanes)]

        def streamed(groups):
            return [(*col, True) for group in groups for col in group]

        near = streamed(own_cols + plane_cols + twin_cols)
        state = match(None, [(mine, own_cols)], shape)
        rest = [(early, own_cols)] if early else []
        state = match(state, rest + [(mine + early, plane_cols)], shape)
        state = match(state, [(mine + early, twin_cols)], shape)
        state = match(state, [(near, [[half_a[:2]]])], shape, half_a[0])
        state = match(state, [([*mine, *early, half_a], corner_cols)], shape)
        state = match(state, [([*mine, *early, half_a], ctwin_cols)], shape)
        best = list(state[: len(line)])
        shift = len(line)
        streams = [(b, (at[0] - shift, *at[1:]), gives) for b, at, gives in near + streamed(corner_cols + ctwin_cols)]
        piece_at = (half_b[0], (0, *half_b[1][1:]))
        late, ours, theirs = match(state[shift:], [(streams, [[piece_at]])], (1, *shape[1:]), half_b[0])
        best.append(late)

        theirs = send(theirs, swap)
        back = [best[0]]
        for value, m in zip(best[1:], maps):
            back.append(send(value, layout.line_return(m)))
        own_best, *others = merge(ours, theirs)
        back.append(own_best)
        for value, d in zip(others, offsets):
            back.append(send(value, backward(layout.plane_move(*d))))
        best = functools.reduce(jnp.maximum, back)
        return jnp.maximum(best, -1.0).reshape(doc_order.shape)

    return jax.shard_map(
        nearest,
        mesh=mesh,
        in_specs=(P(AXES, None), P(AXES)),
        out_specs=P(AXES),
        check_vma=False,
    )
```

```python
import functools

import jax
import jax.numpy as jnp
from jax import lax
from jax.experimental import pallas as pl
from jax.experimental.pallas import tpu as pltpu
from jax.sharding import PartitionSpec as P

AXES = ("row", "col")
CORES = 2
PAD = 8
FAR = 1.0e9
VMEM_GRANT = 16 << 20


class Layout:
    def __init__(self, mesh):
        rows, cols = mesh.shape["row"], mesh.shape["col"]
        self.xs = cols // CORES
        self.ys = self.xs if rows % self.xs == 0 else 1
        self.lines = rows // self.ys

    def index(self, line, y, x, core):
        return ((line * self.ys + y) * self.xs + x) * CORES + core

    def pairs(self, target):
        found = []
        for line in range(self.lines):
            for y in range(self.ys):
                for x in range(self.xs):
                    for core in range(CORES):
                        to = target(line, y, x, core)
                        if to is not None:
                            found.append((self.index(line, y, x, core), self.index(*to)))
        return found

    def plane_move(self, dy, dx):
        return self.pairs(lambda l, y, x, c: (l, (y + dy) % self.ys, (x + dx) % self.xs, c))

    def swap(self):
        return self.pairs(lambda l, y, x, c: (l, y, x, CORES - 1 - c))

    def plane_offsets(self):
        return [(dy, dx) for dy in range(self.ys) for dx in range(self.xs) if dy or dx]

    def line_maps(self):
        maps = []
        for step in range(1, (self.lines + 1) // 2):
            maps.append({i: (i + step) % self.lines for i in range(self.lines)})
        if self.lines % 2 == 0:
            half = self.lines // 2
            maps.append({(i + half if i % 2 == 0 else i): (i if i % 2 == 0 else i + half) for i in range(half)})
        return maps

    def line_move(self, line_map):
        return self.pairs(lambda l, y, x, c: (line_map[l], y, x, c) if l in line_map else None)

    def line_return(self, line_map):
        back = {b: a for a, b in line_map.items()}
        free = [i for i in range(self.lines) if i not in line_map]
        back.update(zip([i for i in range(self.lines) if i not in back], free))
        return self.line_move(back)


def backward(pairs):
    return [(b, a) for a, b in pairs]


def pack_body(pieces, chunk, emb_hbm, order_hbm, out_ref, *refs):
    piece_refs, (emb_ref, order_ref, sems) = refs[: len(pieces)], refs[len(pieces) :]
    n, width = emb_ref.shape
    order_copy = pltpu.make_async_copy(order_hbm, order_ref, sems.at[0])
    order_copy.start()
    copies = []
    for k in range(n // chunk):
        rows = pl.ds(k * chunk, chunk)
        copies.append(pltpu.make_async_copy(emb_hbm.at[rows, :], emb_ref.at[rows, :], sems.at[k + 1]))
        copies[-1].start()
    out_ref[n:, :] = jnp.zeros((PAD, width), jnp.bfloat16)
    order_copy.wait()
    code = order_ref[...].reshape(1, n) + 1
    high = (code >> 8).astype(jnp.float32)
    low = (code & 255).astype(jnp.float32)
    line = lax.broadcasted_iota(jnp.int32, (PAD, n), 0)
    tail = jnp.where(line == 0, high, jnp.where(line == 1, low, 0.0))
    out_ref[n:, :n] = tail.astype(jnp.bfloat16)
    for k in range(n // chunk):
        copies[k].wait()
        rows = slice(k * chunk, (k + 1) * chunk)
        floats = emb_ref[rows, :].astype(jnp.float32)
        scale = lax.rsqrt(jnp.sum(floats * floats, axis=1, keepdims=True) + 1e-06)
        out_ref[rows, :] = (floats * scale).astype(jnp.bfloat16)
    for (start, rows), ref in zip(pieces, piece_refs):
        cut(out_ref, start, rows, ref)


def pack(embeddings, doc_order, pieces):
    n, width = embeddings.shape
    chunk = 128 if n % 128 == 0 else n
    call = pl.pallas_call(
        functools.partial(pack_body, pieces, chunk),
        in_specs=[pl.BlockSpec(memory_space=pltpu.HBM)] * 2,
        out_shape=[pltpu.VMEM((rows + PAD, width), jnp.bfloat16) for rows in (n, *(rows for _, rows in pieces))],
        scratch_shapes=[
            pltpu.VMEM((n, width), jnp.bfloat16),
            pltpu.VMEM((n,), jnp.int32),
            pltpu.SemaphoreType.DMA((n // chunk + 1,)),
        ],
        compiler_params=pltpu.CompilerParams(vmem_limit_bytes=VMEM_GRANT),
        name="pack",
    )
    return call(*(pltpu.with_memory_space_constraint(v, pltpu.HBM) for v in (embeddings, doc_order)))


def cut(ref, start, rows, out_ref):
    n = ref.shape[0] - PAD
    out_ref[:rows, :] = ref[start : start + rows, :]
    out_ref[rows:, :] = jnp.zeros((PAD, ref.shape[1]), jnp.bfloat16)
    out_ref[rows:, :rows] = ref[n:, start : start + rows]


def piece_body(start, rows, ref, out_ref):
    cut(ref, start, rows, out_ref)


def piece(block, start, rows):
    return pl.pallas_call(
        functools.partial(piece_body, start, rows),
        out_shape=pltpu.VMEM((rows + PAD, block.shape[1]), jnp.bfloat16),
        compiler_params=pltpu.CompilerParams(vmem_limit_bytes=VMEM_GRANT),
        name="piece",
    )(*in_vmem([block]))


def lane_orders(ref):
    n = ref.shape[0] - PAD
    tail = ref[n:, :n].astype(jnp.float32)
    order = tail[0:1] * 256.0 + tail[1:2]
    return jnp.where(order == 0.0, FAR, order)


def match_body(tasks, groups, n_blocks, initial, needed, *refs):
    blocks, refs = refs[:n_blocks], refs[n_blocks:]
    count = len(refs) - 1 if initial else len(refs) // 2
    before, after, col_acc = refs[: len(refs) - count - 1], refs[-count - 1 : -1], refs[-1]
    lanes = 128
    for k, ref in enumerate(after):
        ref[...] = jnp.full(ref.shape, -1.0, jnp.float32) if initial else before[k][...]

    def work():
        def units_of(numbers):
            parts = [blocks[k][: blocks[k].shape[0] - PAD, :] for k in numbers]
            return parts[0] if len(parts) == 1 else jnp.concatenate(parts, axis=0)

        def settle(value, block, place):
            orders = lane_orders(blocks[block])
            result, row, lane = place
            at = (slice(row, row + 1), slice(lane, lane + orders.shape[1]))
            after[result][at] = jnp.maximum(after[result][at], jnp.where(orders == FAR, -1.0, value))

        fresh = set()
        for rows, meets in tasks:
            row_units = units_of([row[0] for row in rows])
            sizes = [blocks[row[0]].shape[0] - PAD for row in rows]
            columns = [jnp.broadcast_to(lane_orders(blocks[row[0]]), (lanes, n)).T[:, 0:1] for row, n in zip(rows, sizes)]
            best = [jnp.full((n, lanes), -1.0, jnp.float32) for n in sizes]
            gives = any(row[2] for row in rows)
            for g in meets:
                numbers = [col[0] for col in groups[g]]
                orders = jnp.concatenate([lane_orders(blocks[k]) for k in numbers], axis=1)
                score = lax.dot_general(
                    row_units, units_of(numbers), (((1,), (1,)), ((), ())), preferred_element_type=jnp.float32
                )
                for k in range(0, score.shape[1], lanes):
                    first = 0
                    kept = [col_acc[g, :, k : k + lanes]] if g in fresh else []
                    for r, n in enumerate(sizes):
                        part = score[first : first + n, k : k + lanes]
                        earlier = orders[:, k : k + lanes] < columns[r]
                        best[r] = jnp.maximum(best[r], jnp.where(earlier, part, -1.0))
                        if rows[r][2]:
                            kept.append(jnp.max(jnp.where(earlier, -1.0, part).reshape(n // 8, 8, lanes), axis=0))
                        first += n
                    if gives:
                        col_acc[g, :, k : k + lanes] = functools.reduce(jnp.maximum, kept)
                if gives:
                    fresh.add(g)
            for r, (block, place, _) in enumerate(rows):
                settle(jnp.max(best[r].T, axis=0, keepdims=True), block, place)
        for g in sorted(fresh):
            start = 0
            for block, place in groups[g]:
                n = blocks[block].shape[0] - PAD
                settle(jnp.max(col_acc[g, :, start : start + n], axis=0, keepdims=True), block, place)
                start += n

    if needed is None:
        work()
    else:
        pl.when(jnp.min(lane_orders(blocks[needed])) < FAR)(work)


def in_vmem(values):
    return [pltpu.with_memory_space_constraint(v, pltpu.VMEM) for v in values]


def match(state, tasks, shape, needed=None):
    blocks, groups, plan = [], [], []

    def number(value):
        for k, known in enumerate(blocks):
            if known is value:
                return k
        blocks.append(value)
        return len(blocks) - 1

    for rows, meets in tasks:
        found = []
        for group in meets:
            group = [(number(block), place) for block, place in group]
            if group not in groups:
                groups.append(group)
            found.append(groups.index(group))
        plan.append(([(number(row), *rest) for row, *rest in rows], found))
    rows, chips, n = shape
    width = blocks[0].shape[1]
    widest = max(sum(blocks[col[0]].shape[0] - PAD for col in group) for group in groups)
    pairs = sum(blocks[r[0]].shape[0] * blocks[col[0]].shape[0] for p in plan for r in p[0] for g in p[1] for col in groups[g])
    return pl.pallas_call(
        functools.partial(match_body, plan, groups, len(blocks), state is None, None if needed is None else number(needed)),
        out_shape=[pltpu.VMEM((1, n), jnp.float32)] * rows + [pltpu.VMEM((chips, n), jnp.float32)] * 2,
        scratch_shapes=[pltpu.VMEM((len(groups), 8, widest), jnp.float32)],
        cost_estimate=pl.CostEstimate(flops=2 * pairs * width, bytes_accessed=2 * len(blocks) * n * width, transcendentals=0),
        compiler_params=pltpu.CompilerParams(vmem_limit_bytes=VMEM_GRANT),
    )(*in_vmem([*blocks, *(state or ())]))


def merge_body(ours_ref, theirs_ref, *out_refs):
    value = jnp.maximum(ours_ref[...], theirs_ref[...])
    for k, ref in enumerate(out_refs):
        ref[...] = value[k : k + 1]


def merge(ours, theirs):
    count, n = ours.shape
    return pl.pallas_call(
        merge_body,
        out_shape=[pltpu.VMEM((1, n), jnp.float32)] * count,
        compiler_params=pltpu.CompilerParams(vmem_limit_bytes=VMEM_GRANT),
        name="merge",
    )(*in_vmem([ours, theirs]))


def solution(mesh):
    layout = Layout(mesh)
    maps = layout.line_maps()
    offsets = layout.plane_offsets()

    def send(value, pairs):
        return lax.ppermute(value, AXES, pairs)

    def nearest(embeddings, doc_order):
        n = embeddings.shape[0]
        tile = 128
        pieces = ((0, tile), (tile, n - tile))
        corner_pieces = ((0, n - tile), (n - tile, tile))
        swap = layout.swap()

        own, *parts = pack(embeddings, doc_order, pieces)
        line = [[send(own, layout.line_move(m))] for m in maps[:-1]]
        line.append([send(part, layout.line_move(maps[-1])) for part in parts])
        plane = [send(own, layout.plane_move(*d)) for d in offsets[:-1]]

        dy, dx = offsets[-1]
        routes = [((0, dx), (dy, 0)), ((dy, 0), (0, dx))]
        corner = []
        for k, (start, rows) in enumerate(corner_pieces):
            have, move = routes[k % 2]
            block = piece(plane[offsets.index(have)], start, rows)
            corner.append(send(block, layout.plane_move(*move)))
        twins = [send(block, swap) for block in [own, *plane]]
        corner_twins = [send(block, swap) for block in corner]

        far = len(offsets)
        shape = (len(line) + 1, far + 1, n)
        side_of = [len(line) + 1, len(line) + 2]

        def by_two(blocks, side):
            cols = [(block, (side_of[side], k + 1, 0)) for k, block in enumerate(blocks)]
            return [cols[k : k + 2] for k in range(0, len(cols), 2)]

        own_cols = [[(own, (side_of[0], 0, 0)), (twins[0], (side_of[1], 0, 0))]]
        plane_cols, twin_cols = by_two(plane, 0), by_two(twins[1:], 1)
        corner_cols, ctwin_cols = (
            [[(block, (side_of[side], far, start)) for block, (start, _) in zip(blocks, corner_pieces)]]
            for side, blocks in enumerate((corner, corner_twins))
        )
        lanes = [start for start, _ in pieces]
        mine = [(own, (0, 0, 0), False)]
        early = [(step[0], (k + 1, 0, 0), True) for k, step in enumerate(line[:-1])]
        half_a, half_b = [(block, (len(line), 0, at), True) for block, at in zip(line[-1], lanes)]

        def streamed(groups):
            return [(*col, True) for group in groups for col in group]

        near = streamed(own_cols + plane_cols + twin_cols)
        state = match(None, [(mine, own_cols)], shape)
        rest = [(early, own_cols)] if early else []
        state = match(state, rest + [(mine + early, plane_cols)], shape)
        state = match(state, [(mine + early, twin_cols)], shape)
        state = match(state, [(near, [[half_a[:2]]])], shape, half_a[0])
        state = match(state, [([*mine, *early, half_a], corner_cols)], shape)
        state = match(state, [([*mine, *early, half_a], ctwin_cols)], shape)
        best = list(state[: len(line)])
        shift = len(line)
        streams = [(b, (at[0] - shift, *at[1:]), gives) for b, at, gives in near + streamed(corner_cols + ctwin_cols)]
        piece_at = (half_b[0], (0, *half_b[1][1:]))
        late, ours, theirs = match(state[shift:], [(streams, [[piece_at]])], (1, *shape[1:]), half_b[0])
        best.append(late)

        theirs = send(theirs, swap)
        back = [best[0]]
        for value, m in zip(best[1:], maps):
            back.append(send(value, layout.line_return(m)))
        own_best, *others = merge(ours, theirs)
        back.append(own_best)
        for value, d in zip(others, offsets):
            back.append(send(value, backward(layout.plane_move(*d))))
        best = functools.reduce(jnp.maximum, back)
        return jnp.maximum(best, -1.0).reshape(doc_order.shape)

    return jax.shard_map(
        nearest,
        mesh=mesh,
        in_specs=(P(AXES, None), P(AXES)),
        out_specs=P(AXES),
        check_vma=False,
    )
```

```python
import functools

import jax
import jax.numpy as jnp
from jax import lax
from jax.experimental import pallas as pl
from jax.experimental.pallas import tpu as pltpu
from jax.sharding import PartitionSpec as P

AXES = ("row", "col")
CORES = 2
PAD = 8
FAR = 1.0e9
VMEM_GRANT = 16 << 20


class Layout:
    def __init__(self, mesh):
        rows, cols = mesh.shape["row"], mesh.shape["col"]
        self.xs = cols // CORES
        self.ys = self.xs if rows % self.xs == 0 else 1
        self.lines = rows // self.ys

    def index(self, line, y, x, core):
        return ((line * self.ys + y) * self.xs + x) * CORES + core

    def pairs(self, target):
        found = []
        for line in range(self.lines):
            for y in range(self.ys):
                for x in range(self.xs):
                    for core in range(CORES):
                        to = target(line, y, x, core)
                        if to is not None:
                            found.append((self.index(line, y, x, core), self.index(*to)))
        return found

    def plane_move(self, dy, dx):
        return self.pairs(lambda l, y, x, c: (l, (y + dy) % self.ys, (x + dx) % self.xs, c))

    def swap(self):
        return self.pairs(lambda l, y, x, c: (l, y, x, CORES - 1 - c))

    def plane_offsets(self):
        return [(dy, dx) for dy in range(self.ys) for dx in range(self.xs) if dy or dx]

    def line_maps(self):
        maps = []
        for step in range(1, (self.lines + 1) // 2):
            maps.append({i: (i + step) % self.lines for i in range(self.lines)})
        if self.lines % 2 == 0:
            half = self.lines // 2
            maps.append({(i + half if i % 2 == 0 else i): (i if i % 2 == 0 else i + half) for i in range(half)})
        return maps

    def line_move(self, line_map):
        return self.pairs(lambda l, y, x, c: (line_map[l], y, x, c) if l in line_map else None)

    def line_return(self, line_map):
        back = {b: a for a, b in line_map.items()}
        free = [i for i in range(self.lines) if i not in line_map]
        back.update(zip([i for i in range(self.lines) if i not in back], free))
        return self.line_move(back)


def backward(pairs):
    return [(b, a) for a, b in pairs]


def pack_body(pieces, chunk, emb_hbm, order_hbm, out_ref, *refs):
    piece_refs, (emb_ref, order_ref, sems) = refs[: len(pieces)], refs[len(pieces) :]
    n, width = emb_ref.shape
    order_copy = pltpu.make_async_copy(order_hbm, order_ref, sems.at[0])
    order_copy.start()
    copies = []
    for k in range(n // chunk):
        rows = pl.ds(k * chunk, chunk)
        copies.append(pltpu.make_async_copy(emb_hbm.at[rows, :], emb_ref.at[rows, :], sems.at[k + 1]))
        copies[-1].start()
    out_ref[n:, :] = jnp.zeros((PAD, width), jnp.bfloat16)
    order_copy.wait()
    code = order_ref[...].reshape(1, n) + 1
    high = (code >> 8).astype(jnp.float32)
    low = (code & 255).astype(jnp.float32)
    line = lax.broadcasted_iota(jnp.int32, (PAD, n), 0)
    tail = jnp.where(line == 0, high, jnp.where(line == 1, low, 0.0))
    out_ref[n:, :n] = tail.astype(jnp.bfloat16)
    for k in range(n // chunk):
        copies[k].wait()
        rows = slice(k * chunk, (k + 1) * chunk)
        floats = emb_ref[rows, :].astype(jnp.float32)
        scale = lax.rsqrt(jnp.sum(floats * floats, axis=1, keepdims=True) + 1e-06)
        out_ref[rows, :] = (floats * scale).astype(jnp.bfloat16)
    for (start, rows), ref in zip(pieces, piece_refs):
        cut(out_ref, start, rows, ref)


def pack(embeddings, doc_order, pieces):
    n, width = embeddings.shape
    chunk = n
    call = pl.pallas_call(
        functools.partial(pack_body, pieces, chunk),
        in_specs=[pl.BlockSpec(memory_space=pltpu.HBM)] * 2,
        out_shape=[pltpu.VMEM((rows + PAD, width), jnp.bfloat16) for rows in (n, *(rows for _, rows in pieces))],
        scratch_shapes=[
            pltpu.VMEM((n, width), jnp.bfloat16),
            pltpu.VMEM((n,), jnp.int32),
            pltpu.SemaphoreType.DMA((n // chunk + 1,)),
        ],
        compiler_params=pltpu.CompilerParams(vmem_limit_bytes=VMEM_GRANT),
        name="pack",
    )
    return call(*(pltpu.with_memory_space_constraint(v, pltpu.HBM) for v in (embeddings, doc_order)))


def cut(ref, start, rows, out_ref):
    n = ref.shape[0] - PAD
    out_ref[:rows, :] = ref[start : start + rows, :]
    out_ref[rows:, :] = jnp.zeros((PAD, ref.shape[1]), jnp.bfloat16)
    out_ref[rows:, :rows] = ref[n:, start : start + rows]


def piece_body(start, rows, ref, out_ref):
    cut(ref, start, rows, out_ref)


def piece(block, start, rows):
    return pl.pallas_call(
        functools.partial(piece_body, start, rows),
        out_shape=pltpu.VMEM((rows + PAD, block.shape[1]), jnp.bfloat16),
        compiler_params=pltpu.CompilerParams(vmem_limit_bytes=VMEM_GRANT),
        name="piece",
    )(*in_vmem([block]))


def lane_orders(ref):
    n = ref.shape[0] - PAD
    tail = ref[n:, :n].astype(jnp.float32)
    order = tail[0:1] * 256.0 + tail[1:2]
    return jnp.where(order == 0.0, FAR, order)


def match_body(tasks, groups, n_blocks, initial, needed, *refs):
    blocks, refs = refs[:n_blocks], refs[n_blocks:]
    count = len(refs) - 1 if initial else len(refs) // 2
    before, after, col_acc = refs[: len(refs) - count - 1], refs[-count - 1 : -1], refs[-1]
    lanes = 128
    for k, ref in enumerate(after):
        ref[...] = jnp.full(ref.shape, -1.0, jnp.float32) if initial else before[k][...]

    def work():
        def units_of(numbers):
            parts = [blocks[k][: blocks[k].shape[0] - PAD, :] for k in numbers]
            return parts[0] if len(parts) == 1 else jnp.concatenate(parts, axis=0)

        def settle(value, block, place):
            orders = lane_orders(blocks[block])
            result, row, lane = place
            at = (slice(row, row + 1), slice(lane, lane + orders.shape[1]))
            after[result][at] = jnp.maximum(after[result][at], jnp.where(orders == FAR, -1.0, value))

        fresh = set()
        for rows, meets in tasks:
            row_units = units_of([row[0] for row in rows])
            sizes = [blocks[row[0]].shape[0] - PAD for row in rows]
            columns = [jnp.broadcast_to(lane_orders(blocks[row[0]]), (lanes, n)).T[:, 0:1] for row, n in zip(rows, sizes)]
            best = [jnp.full((n, lanes), -1.0, jnp.float32) for n in sizes]
            gives = any(row[2] for row in rows)
            for g in meets:
                numbers = [col[0] for col in groups[g]]
                orders = jnp.concatenate([lane_orders(blocks[k]) for k in numbers], axis=1)
                score = lax.dot_general(
                    row_units, units_of(numbers), (((1,), (1,)), ((), ())), preferred_element_type=jnp.float32
                )
                for k in range(0, score.shape[1], lanes):
                    first = 0
                    kept = [col_acc[g, :, k : k + lanes]] if g in fresh else []
                    for r, n in enumerate(sizes):
                        part = score[first : first + n, k : k + lanes]
                        earlier = orders[:, k : k + lanes] < columns[r]
                        best[r] = jnp.maximum(best[r], jnp.where(earlier, part, -1.0))
                        if rows[r][2]:
                            kept.append(jnp.max(jnp.where(earlier, -1.0, part).reshape(n // 8, 8, lanes), axis=0))
                        first += n
                    if gives:
                        col_acc[g, :, k : k + lanes] = functools.reduce(jnp.maximum, kept)
                if gives:
                    fresh.add(g)
            for r, (block, place, _) in enumerate(rows):
                settle(jnp.max(best[r].T, axis=0, keepdims=True), block, place)
        for g in sorted(fresh):
            start = 0
            for block, place in groups[g]:
                n = blocks[block].shape[0] - PAD
                settle(jnp.max(col_acc[g, :, start : start + n], axis=0, keepdims=True), block, place)
                start += n

    if needed is None:
        work()
    else:
        pl.when(jnp.min(lane_orders(blocks[needed])) < FAR)(work)


def in_vmem(values):
    return [pltpu.with_memory_space_constraint(v, pltpu.VMEM) for v in values]


def match(state, tasks, shape, needed=None):
    blocks, groups, plan = [], [], []

    def number(value):
        for k, known in enumerate(blocks):
            if known is value:
                return k
        blocks.append(value)
        return len(blocks) - 1

    for rows, meets in tasks:
        found = []
        for group in meets:
            group = [(number(block), place) for block, place in group]
            if group not in groups:
                groups.append(group)
            found.append(groups.index(group))
        plan.append(([(number(row), *rest) for row, *rest in rows], found))
    rows, chips, n = shape
    width = blocks[0].shape[1]
    widest = max(sum(blocks[col[0]].shape[0] - PAD for col in group) for group in groups)
    pairs = sum(blocks[r[0]].shape[0] * blocks[col[0]].shape[0] for p in plan for r in p[0] for g in p[1] for col in groups[g])
    return pl.pallas_call(
        functools.partial(match_body, plan, groups, len(blocks), state is None, None if needed is None else number(needed)),
        out_shape=[pltpu.VMEM((1, n), jnp.float32)] * rows + [pltpu.VMEM((chips, n), jnp.float32)] * 2,
        scratch_shapes=[pltpu.VMEM((len(groups), 8, widest), jnp.float32)],
        cost_estimate=pl.CostEstimate(flops=2 * pairs * width, bytes_accessed=2 * len(blocks) * n * width, transcendentals=0),
        compiler_params=pltpu.CompilerParams(vmem_limit_bytes=VMEM_GRANT),
    )(*in_vmem([*blocks, *(state or ())]))


def final_body(*refs):
    best = functools.reduce(jnp.maximum, [ref[...] for ref in refs[:-1]])
    refs[-1][...] = jnp.maximum(best, -1.0).reshape(refs[-1].shape)


def final(parts):
    return pl.pallas_call(
        final_body,
        out_shape=jax.ShapeDtypeStruct((parts[0].shape[1],), jnp.float32),
        compiler_params=pltpu.CompilerParams(vmem_limit_bytes=VMEM_GRANT),
        name="final",
    )(*in_vmem(parts))


def merge_body(ours_ref, theirs_ref, *out_refs):
    value = jnp.maximum(ours_ref[...], theirs_ref[...])
    for k, ref in enumerate(out_refs):
        ref[...] = value[k : k + 1]


def merge(ours, theirs):
    count, n = ours.shape
    return pl.pallas_call(
        merge_body,
        out_shape=[pltpu.VMEM((1, n), jnp.float32)] * count,
        compiler_params=pltpu.CompilerParams(vmem_limit_bytes=VMEM_GRANT),
        name="merge",
    )(*in_vmem([ours, theirs]))


def solution(mesh):
    layout = Layout(mesh)
    maps = layout.line_maps()
    offsets = layout.plane_offsets()

    def send(value, pairs):
        return lax.ppermute(value, AXES, pairs)

    def nearest(embeddings, doc_order):
        n = embeddings.shape[0]
        tile = 128
        pieces = ((0, tile), (tile, n - tile))
        corner_pieces = ((0, n - tile), (n - tile, tile))
        swap = layout.swap()

        own, *parts = pack(embeddings, doc_order, pieces)
        line = [[send(own, layout.line_move(m))] for m in maps[:-1]]
        line.append([send(part, layout.line_move(maps[-1])) for part in parts])
        plane = [send(own, layout.plane_move(*d)) for d in offsets[:-1]]

        dy, dx = offsets[-1]
        routes = [((0, dx), (dy, 0)), ((dy, 0), (0, dx))]
        corner = []
        for k, (start, rows) in enumerate(corner_pieces):
            have, move = routes[k % 2]
            block = piece(plane[offsets.index(have)], start, rows)
            corner.append(send(block, layout.plane_move(*move)))
        twins = [send(block, swap) for block in [own, *plane]]
        corner_twins = [send(block, swap) for block in corner]

        far = len(offsets)
        shape = (len(line) + 1, far + 1, n)
        side_of = [len(line) + 1, len(line) + 2]

        def by_two(blocks, side):
            cols = [(block, (side_of[side], k + 1, 0)) for k, block in enumerate(blocks)]
            return [cols[k : k + 2] for k in range(0, len(cols), 2)]

        own_cols = [[(own, (side_of[0], 0, 0)), (twins[0], (side_of[1], 0, 0))]]
        plane_cols, twin_cols = by_two(plane, 0), by_two(twins[1:], 1)
        corner_cols, ctwin_cols = (
            [[(block, (side_of[side], far, start)) for block, (start, _) in zip(blocks, corner_pieces)]]
            for side, blocks in enumerate((corner, corner_twins))
        )
        lanes = [start for start, _ in pieces]
        mine = [(own, (0, 0, 0), False)]
        early = [(step[0], (k + 1, 0, 0), True) for k, step in enumerate(line[:-1])]
        half_a, half_b = [(block, (len(line), 0, at), True) for block, at in zip(line[-1], lanes)]

        def streamed(groups):
            return [(*col, True) for group in groups for col in group]

        near = streamed(own_cols + plane_cols + twin_cols)
        state = match(None, [(mine, own_cols)], shape)
        rest = [(early, own_cols)] if early else []
        state = match(state, rest + [(mine + early, plane_cols)], shape)
        state = match(state, [(mine + early, twin_cols)], shape)
        state = match(state, [(near, [[half_a[:2]]])], shape, half_a[0])
        state = match(state, [([*mine, *early, half_a], corner_cols)], shape)
        state = match(state, [([*mine, *early, half_a], ctwin_cols)], shape)
        best = list(state[: len(line)])
        shift = len(line)
        streams = [(b, (at[0] - shift, *at[1:]), gives) for b, at, gives in near + streamed(corner_cols + ctwin_cols)]
        piece_at = (half_b[0], (0, *half_b[1][1:]))
        late, ours, theirs = match(state[shift:], [(streams, [[piece_at]])], (1, *shape[1:]), half_b[0])
        best.append(late)

        theirs = send(theirs, swap)
        back = [best[0]]
        for value, m in zip(best[1:], maps):
            back.append(send(value, layout.line_return(m)))
        own_best, *others = merge(ours, theirs)
        back.append(own_best)
        for value, d in zip(others, offsets):
            back.append(send(value, backward(layout.plane_move(*d))))
        return final(back)

    return jax.shard_map(
        nearest,
        mesh=mesh,
        in_specs=(P(AXES, None), P(AXES)),
        out_specs=P(AXES),
        check_vma=False,
    )
```
